32 devices in a mesh: tm: 8 (over z, y), rows: 4 (over x, core).
Axes of the slice: x: 2, y: 2, z: 4, core: 2. Of those that a mesh axis runs over, the one named last changes fastest.
Arguments:
- upstream: bfloat16 [32, 32, 128, 128], P('tm', 'rows'), may hold values from -6 to 6
- saved_first: bfloat16 [32, 32, 128, 128], P('tm', 'rows'), may hold values from -8 to 8
- saved_second: bfloat16 [32, 32, 128, 128], P('tm', 'rows'), may hold values from -8 to 8
- weight_first: bfloat16 [3456, 128], replicated, may hold values from -0.109375 to 0.109375
- weight_second: bfloat16 [3456, 128], replicated, may hold values from -0.109375 to 0.109375
Outputs:
- grad_input: bfloat16 [32, 32, 128, 128], P('tm', 'rows')
- wgrad_first: float32 [3456, 128], P('tm')
- wgrad_second: float32 [3456, 128], P('tm')
The draws below stay inside these ranges and needn't reach their ends.
All inputs are finite; a program needn't handle non-finite values.
Results may differ from the reference program's by a relative error of at most 0.005.
Values may be sent and summed in bfloat16 or wider, within the bound.
A program may use at most 64 MiB of HBM per device.

```python
import math
import jax
import jax.numpy as jnp
from jax import lax

CH = 128
COLS = 128
NF = 32
NR = 32


def draw_upstream(key, part):
    shape = (NF, NR, COLS, CH)
    offset = 4.0 / math.sqrt(NF * NR * COLS)
    values = jnp.clip(jax.random.normal(key, shape, jnp.float32), -5.9, 5.9)
    return jnp.clip(values + offset, -6.0, 6.0).astype(jnp.bfloat16)


def level_of(stream_key, extent, split, least, top_value):
    factor_of, own = 1.0, jax.random.fold_in(stream_key, 6)
    for position, parts in split:
        draws = jnp.exp(jax.random.uniform(jax.random.fold_in(own, position), (parts,), jnp.float32, least / len(split), top_value / len(split)))
        factor_of = factor_of * jnp.repeat(draws, extent[position] // parts).reshape([-1 if axis == position else 1 for axis in range(len(extent))])
    return factor_of


def centred(rng, shape, deviation, most, cuts=(), kind=jnp.bfloat16):
    array = deviation * jax.random.normal(rng, shape, jnp.float32)
    if cuts:
        array = array * level_of(rng, shape, cuts, -0.22, 0.18)
    return jnp.clip(array, -most, most).astype(kind)


def setup_inputs(seed: int = 0) -> dict:
    seeds = jax.random.split(jax.random.key(seed), 6)
    return {
        "upstream": draw_upstream(jax.random.fold_in(seeds[5], 71), 0),
        "saved_first": centred(seeds[1], (NF, NR, COLS, CH), 1.5, 8.0, ((0, 8), (1, 4))),
        "saved_second": centred(seeds[2], (NF, NR, COLS, CH), 1.5, 8.0, ((0, 8), (1, 4))),
        "weight_first": centred(seeds[3], (27 * CH, CH), (27 * CH) ** -0.5, 0.109375),
        "weight_second": centred(seeds[4], (27 * CH, CH), (27 * CH) ** -0.5, 0.109375),
    }


def silu_slope(value):
    sigma = jax.nn.sigmoid(value)
    return sigma * (1.0 + value * (1.0 - sigma))

def taps_frame(padded, frame, height, width):
    slab = lax.dynamic_slice_in_dim(padded, frame, 3, 0)
    pieces = []
    for shift_t in range(3):
        for shift_r in range(3):
            for shift_c in range(3):
                pieces.append(slab[2 - shift_t, 2 - shift_r:2 - shift_r + height, 2 - shift_c:2 - shift_c + width])
    return jnp.concatenate(pieces, axis=-1).reshape(height * width, -1)

def layer_back(grad_out, saved, weight):
    frames, height, width, chans = grad_out.shape
    padded = jnp.pad(grad_out, ((0, 2), (1, 1), (1, 1), (0, 0)))
    flipped = weight.reshape(27, chans, chans).transpose(0, 2, 1).reshape(27 * chans, chans)
    active = jax.nn.silu(saved.astype(jnp.float32)).astype(jnp.bfloat16)

    def one_frame(total, frame):
        columns = taps_frame(padded, frame, height, width)
        spread = jnp.dot(columns, flipped, preferred_element_type=jnp.float32)
        local_act = lax.dynamic_index_in_dim(active, frame, 0, keepdims=False).reshape(height * width, chans)
        total = total + jnp.dot(local_act.T, columns, preferred_element_type=jnp.float32)
        local_saved = lax.dynamic_index_in_dim(saved, frame, 0, keepdims=False).astype(jnp.float32)
        result = (spread.reshape(height, width, chans) * silu_slope(local_saved)).astype(jnp.bfloat16)
        return (total, result)
    start = jnp.zeros((chans, 27 * chans), jnp.float32)
    total, grads = lax.scan(one_frame, start, jnp.arange(frames, dtype=jnp.int32))
    wsum = total.reshape(chans, 27, chans).transpose(1, 0, 2).reshape(27 * chans, chans)
    return (grads, wsum)

def reference(upstream, saved_first, saved_second, weight_first, weight_second):
    grad_mid, wsum_second = layer_back(upstream, saved_second, weight_second)
    grad_input, wsum_first = layer_back(grad_mid, saved_first, weight_first)
    factor = 1.0 / math.sqrt(upstream.shape[0] * upstream.shape[1] * upstream.shape[2])
    return (grad_input, wsum_first * factor, wsum_second * factor)
```

```python
import functools
import math

import jax
import jax.numpy as jnp
from jax import lax
from jax.experimental import pallas as pl
from jax.experimental.pallas import tpu as pltpu
from jax.sharding import PartitionSpec as P

F32, BF16 = jnp.float32, jnp.bfloat16
VMEM_LIMIT = 60 * 1024 * 1024
MESH = pl.DeviceIdType.MESH


def plan(slots, bands, depth):
    share = depth // slots
    wire, unit = (BF16, 16) if share % 16 == 0 else (F32, 8)
    lanes = bands // 2
    chunk = -(-share // (bands * unit)) * unit
    return share, wire, unit, lanes, chunk, lanes * chunk


def whole_kernel(
    slots, bands, factor,
    up_hbm, first_hbm, second_hbm, weight_first_hbm, weight_second_hbm,
    out_ref, grad_first_ref, grad_second_ref,
    up, saved, weights, mid, wide, above, below, later, later_above, later_below, kernels, active, total,
    core_out, core_in, cross_out, cross_in, slot_sum, slot_out, slot_in, band_out, band_in,
    load_sem, row_send, row_recv, late_send, late_recv, edge_send, edge_recv,
    core_send, core_recv, cross_send, cross_recv, slot_send, slot_recv, band_send, band_recv,
):
    frames, height, width, chans = up.shape
    depth = 27 * chans
    share, wire, unit, lanes, chunk, half_rows = plan(slots, bands, depth)
    t, r = lax.axis_index("tm"), lax.axis_index("rows")
    core, lane = lax.rem(r, 2), r // 2
    has_above, has_below = r > 0, r < bands - 1
    has_prev, has_later = t > 0, t < slots - 1

    def remote(src, dst, send, recv, where):
        return pltpu.make_async_remote_copy(
            src_ref=src, dst_ref=dst, send_sem=send, recv_sem=recv, device_id=where, device_id_type=MESH
        )

    loads = [
        pltpu.make_async_copy(src, dst, load_sem.at[i])
        for i, (src, dst) in enumerate((
            (up_hbm, up), (weight_second_hbm, weights.at[1]), (second_hbm, saved.at[1]),
            (first_hbm, saved.at[0]), (weight_first_hbm, weights.at[0]),
        ))
    ]
    for load in loads:
        load.start()
    barrier = pltpu.get_barrier_semaphore()
    for step in range(1, bands):
        pl.semaphore_signal(barrier, inc=1, device_id=(t, lax.rem(r + step, bands)), device_id_type=MESH)
    for step in range(1, slots):
        pl.semaphore_signal(barrier, inc=1, device_id=(lax.rem(t + step, slots), r), device_id_type=MESH)
    loads[0].wait()
    pl.semaphore_wait(barrier, bands + slots - 2)

    def row_up(layer, grad, low, count, index):
        part = pl.ds(low, count)
        return remote(grad.at[part, 0], below.at[layer, part], row_send.at[layer, index, 0], row_recv.at[layer, index, 0], (t, r - 1))

    def row_down(layer, grad, low, count, index):
        part = pl.ds(low, count)
        return remote(grad.at[part, height - 1], above.at[layer, part], row_send.at[layer, index, 1], row_recv.at[layer, index, 1], (t, r + 1))

    def late(layer, grad, frame):
        return remote(grad.at[frame], later.at[layer, frame], late_send.at[layer, frame], late_recv.at[layer, frame], (t - 1, r))

    def edge_up(layer, frame):
        return remote(later.at[layer, frame, 0], later_below.at[layer, frame], edge_send.at[layer, frame, 0], edge_recv.at[layer, frame, 0], (t, r - 1))

    def edge_down(layer, frame):
        return remote(later.at[layer, frame, height - 1], later_above.at[layer, frame], edge_send.at[layer, frame, 1], edge_recv.at[layer, frame, 1], (t, r + 1))

    def when(flag, *actions):
        @pl.when(flag)
        def _():
            for action in actions:
                action()

    def send_rows(layer, grad, low, count, index):
        when(has_above, lambda: row_up(layer, grad, low, count, index).start())
        when(has_below, lambda: row_down(layer, grad, low, count, index).start())

    def send_late(layer, grad):
        when(has_prev, *[lambda f=f: late(layer, grad, f).start() for f in range(2)])

    place = lax.broadcasted_iota(jnp.int32, (width, chans), 0)

    def fill_row(layer, value, frame, row):
        spread = value.astype(F32)
        after = jnp.where(place == width - 1, 0.0, pltpu.roll(spread, width - 1, 0)).astype(BF16)
        before = jnp.where(place == 0, 0.0, pltpu.roll(spread, 1, 0)).astype(BF16)
        lines = pl.ds(row * width, width) if isinstance(row, int) else pl.ds(pl.multiple_of(row * width, width), width)
        wide[layer, frame, lines, pl.ds(0, chans)] = after
        wide[layer, frame, lines, pl.ds(chans, chans)] = value
        wide[layer, frame, lines, pl.ds(2 * chans, chans)] = before

    def zero_row(layer, frame, row):
        wide[layer, frame, pl.ds(row * width, width), :] = jnp.zeros((width, 3 * chans), BF16)

    def fill_frames(layer, grad, low, high, base=0):
        def one(row, carry):
            for frame in range(low, high):
                fill_row(layer, grad[frame - base, row], frame, row + 1)
            return carry

        lax.fori_loop(0, height, one, 0)

    def take_rows(layer, grad, low, count, index):
        def got_above():
            row_down(layer, grad, low, count, index).wait_recv()
            for frame in range(low, low + count):
                fill_row(layer, above[layer, frame], frame, 0)

        def got_below():
            row_up(layer, grad, low, count, index).wait_recv()
            for frame in range(low, low + count):
                fill_row(layer, below[layer, frame], frame, height + 1)

        when(has_above, got_above)
        when(has_below, got_below)
        when(jnp.logical_not(has_above), *[lambda f=f: zero_row(layer, f, 0) for f in range(low, low + count)])
        when(jnp.logical_not(has_below), *[lambda f=f: zero_row(layer, f, height + 1) for f in range(low, low + count)])

    def take_late(layer, grad):
        def forward(frame):
            late(layer, grad, frame).wait_recv()
            when(has_above, lambda: edge_up(layer, frame).start())
            when(has_below, lambda: edge_down(layer, frame).start())
            fill_frames(layer, later.at[layer], frames + frame, frames + frame + 1, base=frames)

        def edges(frame):
            def got_above():
                edge_down(layer, frame).wait_recv()
                fill_row(layer, later_above[layer, frame], frames + frame, 0)

            def got_below():
                edge_up(layer, frame).wait_recv()
                fill_row(layer, later_below[layer, frame], frames + frame, height + 1)

            when(has_above, got_above)
            when(has_below, got_below)
            when(jnp.logical_not(has_above), lambda: zero_row(layer, frames + frame, 0))
            when(jnp.logical_not(has_below), lambda: zero_row(layer, frames + frame, height + 1))

        when(has_later, *[lambda f=f: forward(f) for f in range(2)], *[lambda f=f: edges(f) for f in range(2)])

        @pl.when(jnp.logical_not(has_later))
        def _():
            for frame in range(2):
                wide[layer, frames + frame] = jnp.zeros(wide.shape[2:], BF16)

    def make_kernels(layer):
        span = 9 * chans
        for half in range(2):
            for j in range(4):
                p = 2 + half - j
                for tap in range(9):
                    block = (
                        weights[layer, pl.ds((9 * p + tap) * chans, chans), :]
                        if 0 <= p < 3
                        else jnp.zeros((chans, chans), BF16)
                    )
                    kernels[layer, pl.ds(half * chans, chans), pl.ds(j * span + tap * chans, chans)] = block

    def make_active(layer):
        def one(frame, carry):
            for row in range(height):
                value = saved[layer, frame, row].astype(F32)
                act = value * jax.nn.sigmoid(value)
                lines = pl.ds(pl.multiple_of(frame * chans, chans), chans)
                active[layer, lines, pl.ds(row * width, width)] = act.T.astype(BF16)
            return carry

        lax.fori_loop(0, frames, one, 0)

    step_rows = math.gcd(4, height)
    lines = step_rows * width

    def spread(layer, pair, target):
        def one(index, carry):
            parts = [
                wide[layer, 2 * pair + j, pl.ds(pl.multiple_of(index * lines + (2 - q) * width, width), lines), :]
                for j in range(4)
                for q in range(3)
            ]
            sums = lax.dot_general(
                jnp.concatenate(parts, axis=1), kernels[layer], (((1,), (1,)), ((), ())), preferred_element_type=F32
            )
            for half in range(2):
                rows = pl.ds(index * step_rows, step_rows)
                value = saved[layer, 2 * pair + half, rows].reshape(lines, chans).astype(F32)
                sigma = jax.nn.sigmoid(value)
                slope = sigma * (1.0 + value * (1.0 - sigma))
                result = sums[:, half * chans : (half + 1) * chans] * slope
                target[2 * pair + half, rows] = result.astype(BF16).reshape(step_rows, width, chans)
            return carry

        lax.fori_loop(0, height // step_rows, one, 0)

    def wsum(layer, frame):
        low, high = max(0, frame - 2), min(frames, frame + 1)
        acts = active[layer, pl.ds(low * chans, (high - low) * chans), :]
        part = jnp.concatenate([wide[layer, frame, pl.ds((2 - q) * width, height * width), :] for q in range(3)], axis=1)
        sums = jnp.dot(acts, part, preferred_element_type=F32)
        for s in range(low, high):
            p = s + 2 - frame
            for tap in range(9):
                rows = pl.ds((9 * p + tap) * chans, chans)
                block = sums[(s - low) * chans : (s - low + 1) * chans, tap * chans : (tap + 1) * chans]
                total[layer, rows, :] = block if s == 0 else total[layer, rows, :] + block

    half_at = lambda which: which * (share - half_rows)
    aligned = lambda value: pl.multiple_of(value, unit)

    def core_copy(layer):
        return remote(core_out.at[layer], core_in.at[layer], core_send.at[layer], core_recv.at[layer], (t, 2 * lane + 1 - core))

    def reduce_core(layer):
        for slot in range(slots):
            lines = pl.ds(aligned(slot * share + half_at(1 - core)), half_rows)
            core_out[layer, slot] = total[layer, lines, :].astype(wire)
        core_copy(layer).start()

    def cross_copy(layer, step):
        to = lax.rem(lane + step, lanes)
        src = cross_out.at[layer, :, pl.ds(aligned(to * chunk), chunk)]
        return remote(src, cross_in.at[layer, step - 1], cross_send.at[layer, step - 1], cross_recv.at[layer, step - 1], (t, 2 * to + core))

    def reduce_cross(layer):
        core_copy(layer).wait_recv()
        for slot in range(slots):
            lines = pl.ds(aligned(slot * share + half_at(core)), half_rows)
            cross_out[layer, slot] = (total[layer, lines, :] + core_in[layer, slot].astype(F32)).astype(wire)
        for step in range(1, lanes):
            cross_copy(layer, step).start()

    def slot_copy(layer, step):
        to = lax.rem(t + step, slots)
        return remote(slot_out.at[layer, to], slot_in.at[layer, step - 1], slot_send.at[layer, step - 1], slot_recv.at[layer, step - 1], (to, r))

    def reduce_slots(layer):
        for step in range(1, lanes):
            cross_copy(layer, step).wait_recv()
        for slot in range(slots):
            lines = pl.ds(aligned(slot * share + half_at(core) + lane * chunk), chunk)
            mine = pl.ds(aligned(lane * chunk), chunk)
            value = total[layer, lines, :] + core_in[layer, slot, mine, :].astype(F32)
            for step in range(1, lanes):
                value = value + cross_in[layer, step - 1, slot].astype(F32)
            slot_sum[layer, slot] = value
            slot_out[layer, slot] = value.astype(wire)
        for step in range(1, slots):
            slot_copy(layer, step).start()

    def band_copy(layer, step):
        to = lax.rem(r + step, bands)
        return remote(band_out.at[layer], band_in.at[layer, step - 1], band_send.at[layer, step - 1], band_recv.at[layer, step - 1], (t, to))

    def reduce_bands(layer):
        for step in range(1, slots):
            slot_copy(layer, step).wait_recv()
        value = slot_sum[layer, t]
        for step in range(1, slots):
            value = value + slot_in[layer, step - 1].astype(F32)
        band_out[layer] = value * factor
        for step in range(1, bands):
            band_copy(layer, step).start()

    def band_lines(band):
        return pl.ds(aligned(half_at(lax.rem(band, 2)) + (band // 2) * chunk), chunk)

    def finish(layer, target):
        target[band_lines(r), :] = band_out[layer]
        for step in range(1, bands):
            band_copy(layer, step).wait_recv()
            target[band_lines(lax.rem(r - step + bands, bands)), :] = band_in[layer, step - 1]

    send_rows(1, up, 0, frames, 0)
    send_late(1, up)
    fill_frames(1, up, 0, frames)
    loads[1].wait()
    make_kernels(1)
    take_rows(1, up, 0, frames, 0)
    loads[2].wait()
    spread(1, 0, mid)
    send_late(0, mid)
    send_rows(0, mid, 0, 2, 0)
    make_active(1)
    for frame in range(frames):
        wsum(1, frame)
    loads[3].wait()
    loads[4].wait()
    make_kernels(0)
    make_active(0)
    fill_frames(0, mid, 0, 2)
    take_late(1, up)
    for pair in range(1, frames // 2):
        spread(1, pair, mid)
        send_rows(0, mid, 2 * pair, 2, pair)
    for frame in range(frames, frames + 2):
        wsum(1, frame)
    reduce_core(1)

    fill_frames(0, mid, 2, frames)
    for pair in range(frames // 2):
        take_rows(0, mid, 2 * pair, 2, pair)
    reduce_cross(1)
    for frame in range(frames):
        wsum(0, frame)
    reduce_slots(1)
    take_late(0, mid)
    for frame in range(frames, frames + 2):
        wsum(0, frame)
    reduce_core(0)
    reduce_bands(1)
    spread(0, 0, out_ref)
    reduce_cross(0)
    for pair in range(1, frames // 2):
        spread(0, pair, out_ref)
    finish(1, grad_second_ref)
    reduce_slots(0)
    reduce_bands(0)
    finish(0, grad_first_ref)

    def sent(*copies):
        for copy in copies:
            copy.wait_send()

    when(has_above, lambda: sent(row_up(1, up, 0, frames, 0), *[row_up(0, mid, 2 * p, 2, p) for p in range(frames // 2)]))
    when(has_below, lambda: sent(row_down(1, up, 0, frames, 0), *[row_down(0, mid, 2 * p, 2, p) for p in range(frames // 2)]))
    when(has_prev, lambda: sent(*[late(1, up, f) for f in range(2)], *[late(0, mid, f) for f in range(2)]))
    for flag, copy in ((has_above, edge_up), (has_below, edge_down)):
        when(jnp.logical_and(has_later, flag), lambda copy=copy: sent(*[copy(layer, f) for layer in range(2) for f in range(2)]))
    for layer in range(2):
        sent(core_copy(layer))
        sent(*[cross_copy(layer, step) for step in range(1, lanes)])
        sent(*[slot_copy(layer, step) for step in range(1, slots)])
        sent(*[band_copy(layer, step) for step in range(1, bands)])


def body(upstream, saved_first, saved_second, weight_first, weight_second):
    slots, bands = lax.axis_size("tm"), lax.axis_size("rows")
    frames, height, width, chans = upstream.shape
    depth = 27 * chans
    share, wire, unit, lanes, chunk, half_rows = plan(slots, bands, depth)
    factor = 1.0 / math.sqrt(frames * slots * height * bands * width)
    pairs = frames // 2
    vmem, dma = pltpu.VMEM, pltpu.SemaphoreType.DMA
    scratch = [
        vmem((frames, height, width, chans), BF16),
        vmem((2, frames, height, width, chans), BF16),
        vmem((2, depth, chans), BF16),
        vmem((frames, height, width, chans), BF16),
        vmem((2, frames + 2, (height + 2) * width, 3 * chans), BF16),
        vmem((2, frames, width, chans), BF16),
        vmem((2, frames, width, chans), BF16),
        vmem((2, 2, height, width, chans), BF16),
        vmem((2, 2, width, chans), BF16),
        vmem((2, 2, width, chans), BF16),
        vmem((2, 2 * chans, 36 * chans), BF16),
        vmem((2, frames * chans, height * width), BF16),
        vmem((2, depth, chans), F32),
        vmem((2, slots, half_rows, chans), wire),
        vmem((2, slots, half_rows, chans), wire),
        vmem((2, slots, half_rows, chans), wire),
        vmem((2, max(1, lanes - 1), slots, chunk, chans), wire),
        vmem((2, slots, chunk, chans), F32),
        vmem((2, slots, chunk, chans), wire),
        vmem((2, slots - 1, chunk, chans), wire),
        vmem((2, chunk, chans), F32),
        vmem((2, bands - 1, chunk, chans), F32),
        dma((5,)),
        dma((2, pairs, 2)), dma((2, pairs, 2)),
        dma((2, 2)), dma((2, 2)),
        dma((2, 2, 2)), dma((2, 2, 2)),
        dma((2,)), dma((2,)),
        dma((2, max(1, lanes - 1))), dma((2, max(1, lanes - 1))),
        dma((2, slots - 1)), dma((2, slots - 1)),
        dma((2, bands - 1)), dma((2, bands - 1)),
    ]
    return pl.pallas_call(
        functools.partial(whole_kernel, slots, bands, factor),
        out_shape=[
            jax.ShapeDtypeStruct(upstream.shape, BF16),
            jax.ShapeDtypeStruct((share, chans), F32),
            jax.ShapeDtypeStruct((share, chans), F32),
        ],
        in_specs=[pl.BlockSpec(memory_space=pl.ANY)] * 5,
        out_specs=[pl.BlockSpec(memory_space=pltpu.VMEM)] * 3,
        scratch_shapes=scratch,
        compiler_params=pltpu.CompilerParams(vmem_limit_bytes=VMEM_LIMIT, collective_id=0, has_side_effects=True),
        name="whole",
    )(upstream, saved_first, saved_second, weight_first, weight_second)


def solution(mesh):
    grid = P("tm", "rows", None, None)
    return jax.shard_map(
        body,
        mesh=mesh,
        in_specs=(grid, grid, grid, P(), P()),
        out_specs=(grid, P("tm", None), P("tm", None)),
        check_vma=False,
    )
```

```python
import functools
import math

import jax
import jax.numpy as jnp
from jax import lax
from jax.experimental import pallas as pl
from jax.experimental.pallas import tpu as pltpu
from jax.sharding import PartitionSpec as P

F32, BF16 = jnp.float32, jnp.bfloat16
VMEM_LIMIT = 52 * 1024 * 1024
MESH = pl.DeviceIdType.MESH


def plan(slots, bands, depth):
    share = depth // slots
    wire, unit = (BF16, 16) if share % 16 == 0 else (F32, 8)
    lanes = bands // 2
    chunk = -(-share // (bands * unit)) * unit
    return share, wire, unit, lanes, chunk, lanes * chunk


def whole_kernel(
    slots, bands, factor,
    up_hbm, first_hbm, second_hbm, weight_first_hbm, weight_second_hbm,
    out_ref, grad_first_ref, grad_second_ref,
    up, saved, weights, mid, wide, above, below, later, later_above, later_below, kernels, active, total,
    core_out, core_in, cross_out, cross_in, slot_sum, slot_out, slot_in, band_in,
    load_sem, row_send, row_recv, late_send, late_recv, edge_send, edge_recv,
    core_send, core_recv, cross_send, cross_recv, slot_send, slot_recv, band_send, band_recv,
):
    frames, height, width, chans = up.shape
    depth = 27 * chans
    share, wire, unit, lanes, chunk, half_rows = plan(slots, bands, depth)
    t, r = lax.axis_index("tm"), lax.axis_index("rows")
    core, lane = lax.rem(r, 2), r // 2
    has_above, has_below = r > 0, r < bands - 1
    has_prev, has_later = t > 0, t < slots - 1

    def remote(src, dst, send, recv, where):
        return pltpu.make_async_remote_copy(
            src_ref=src, dst_ref=dst, send_sem=send, recv_sem=recv, device_id=where, device_id_type=MESH
        )

    loads = [
        pltpu.make_async_copy(src, dst, load_sem.at[i])
        for i, (src, dst) in enumerate((
            (up_hbm, up), (weight_second_hbm, weights.at[1]), (second_hbm, saved.at[1]),
            (first_hbm, saved.at[0]), (weight_first_hbm, weights.at[0]),
        ))
    ]
    for load in loads:
        load.start()
    barrier = pltpu.get_barrier_semaphore()
    for step in range(1, bands):
        pl.semaphore_signal(barrier, inc=1, device_id=(t, lax.rem(r + step, bands)), device_id_type=MESH)
    for step in range(1, slots):
        pl.semaphore_signal(barrier, inc=1, device_id=(lax.rem(t + step, slots), r), device_id_type=MESH)
    loads[0].wait()
    pl.semaphore_wait(barrier, bands + slots - 2)

    def row_up(layer, grad, low, count, index):
        part = pl.ds(low, count)
        return remote(grad.at[part, 0], below.at[layer, part], row_send.at[layer, index, 0], row_recv.at[layer, index, 0], (t, r - 1))

    def row_down(layer, grad, low, count, index):
        part = pl.ds(low, count)
        return remote(grad.at[part, height - 1], above.at[layer, part], row_send.at[layer, index, 1], row_recv.at[layer, index, 1], (t, r + 1))

    def late(layer, grad, frame):
        return remote(grad.at[frame], later.at[layer, frame], late_send.at[layer, frame], late_recv.at[layer, frame], (t - 1, r))

    def edge_up(layer, frame):
        return remote(later.at[layer, frame, 0], later_below.at[layer, frame], edge_send.at[layer, frame, 0], edge_recv.at[layer, frame, 0], (t, r - 1))

    def edge_down(layer, frame):
        return remote(later.at[layer, frame, height - 1], later_above.at[layer, frame], edge_send.at[layer, frame, 1], edge_recv.at[layer, frame, 1], (t, r + 1))

    def when(flag, *actions):
        @pl.when(flag)
        def _():
            for action in actions:
                action()

    def send_rows(layer, grad, low, count, index):
        when(has_above, lambda: row_up(layer, grad, low, count, index).start())
        when(has_below, lambda: row_down(layer, grad, low, count, index).start())

    def send_late(layer, grad):
        when(has_prev, *[lambda f=f: late(layer, grad, f).start() for f in range(2)])

    place = lax.broadcasted_iota(jnp.int32, (width, chans), 0)

    def fill_row(layer, value, frame, row):
        spread = value.astype(F32)
        after = jnp.where(place == width - 1, 0.0, pltpu.roll(spread, width - 1, 0)).astype(BF16)
        before = jnp.where(place == 0, 0.0, pltpu.roll(spread, 1, 0)).astype(BF16)
        lines = pl.ds(row * width, width) if isinstance(row, int) else pl.ds(pl.multiple_of(row * width, width), width)
        wide[layer, frame, lines, pl.ds(0, chans)] = after
        wide[layer, frame, lines, pl.ds(chans, chans)] = value
        wide[layer, frame, lines, pl.ds(2 * chans, chans)] = before

    def zero_row(layer, frame, row):
        wide[layer, frame, pl.ds(row * width, width), :] = jnp.zeros((width, 3 * chans), BF16)

    def fill_frames(layer, grad, low, high, base=0):
        def one(row, carry):
            for frame in range(low, high):
                fill_row(layer, grad[frame - base, row], frame, row + 1)
            return carry

        lax.fori_loop(0, height, one, 0)

    def take_rows(layer, grad, low, count, index):
        def got_above():
            row_down(layer, grad, low, count, index).wait_recv()
            for frame in range(low, low + count):
                fill_row(layer, above[layer, frame], frame, 0)

        def got_below():
            row_up(layer, grad, low, count, index).wait_recv()
            for frame in range(low, low + count):
                fill_row(layer, below[layer, frame], frame, height + 1)

        when(has_above, got_above)
        when(has_below, got_below)
        when(jnp.logical_not(has_above), *[lambda f=f: zero_row(layer, f, 0) for f in range(low, low + count)])
        when(jnp.logical_not(has_below), *[lambda f=f: zero_row(layer, f, height + 1) for f in range(low, low + count)])

    def forward_late(layer, grad):
        def forward(frame):
            late(layer, grad, frame).wait_recv()
            when(has_above, lambda: edge_up(layer, frame).start())
            when(has_below, lambda: edge_down(layer, frame).start())
            fill_frames(layer, later.at[layer], frames + frame, frames + frame + 1, base=frames)

        when(has_later, *[lambda f=f: forward(f) for f in range(2)])

        @pl.when(jnp.logical_not(has_later))
        def _():
            for frame in range(2):
                wide[layer, frames + frame] = jnp.zeros(wide.shape[2:], BF16)

    def take_edges(layer):
        def edges(frame):
            def got_above():
                edge_down(layer, frame).wait_recv()
                fill_row(layer, later_above[layer, frame], frames + frame, 0)

            def got_below():
                edge_up(layer, frame).wait_recv()
                fill_row(layer, later_below[layer, frame], frames + frame, height + 1)

            when(has_above, got_above)
            when(has_below, got_below)
            when(jnp.logical_not(has_above), lambda: zero_row(layer, frames + frame, 0))
            when(jnp.logical_not(has_below), lambda: zero_row(layer, frames + frame, height + 1))

        when(has_later, *[lambda f=f: edges(f) for f in range(2)])

    def make_kernels(layer):
        span = 9 * chans
        for half in range(2):
            for j in range(4):
                p = 2 + half - j
                for tap in range(9):
                    block = (
                        weights[layer, pl.ds((9 * p + tap) * chans, chans), :]
                        if 0 <= p < 3
                        else jnp.zeros((chans, chans), BF16)
                    )
                    kernels[layer, pl.ds(half * chans, chans), pl.ds(j * span + tap * chans, chans)] = block

    def make_active(layer):
        def one(frame, carry):
            for row in range(height):
                value = saved[layer, frame, row].astype(F32)
                act = value * jax.nn.sigmoid(value)
                lines = pl.ds(pl.multiple_of(frame * chans, chans), chans)
                active[layer, lines, pl.ds(row * width, width)] = act.T.astype(BF16)
            return carry

        lax.fori_loop(0, frames, one, 0)

    step_rows = math.gcd(4, height)
    lines = step_rows * width

    def spread(layer, pair, target, low=0, high=height // step_rows):
        def one(index, carry):
            pieces = [
                wide[layer, 2 * pair + j, pl.ds(pl.multiple_of(index * lines + (2 - q) * width, width), lines), :]
                for j in range(4)
                for q in range(3)
            ]
            sums = lax.dot_general(
                jnp.concatenate(pieces, axis=1), kernels[layer], (((1,), (1,)), ((), ())), preferred_element_type=F32
            )
            for half in range(2):
                rows = pl.ds(index * step_rows, step_rows)
                value = saved[layer, 2 * pair + half, rows].reshape(lines, chans).astype(F32)
                sigma = jax.nn.sigmoid(value)
                slope = sigma * (1.0 + value * (1.0 - sigma))
                result = sums[:, half * chans : (half + 1) * chans] * slope
                target[2 * pair + half, rows] = result.astype(BF16).reshape(step_rows, width, chans)
            return carry

        lax.fori_loop(low, high, one, 0)

    def wsum(layer, frame, taps=(0, 1, 2)):
        low, high = max(0, frame - 2), min(frames, frame + 1)
        acts = active[layer, pl.ds(low * chans, (high - low) * chans), :]
        part = jnp.concatenate([wide[layer, frame, pl.ds((2 - q) * width, height * width), :] for q in taps], axis=1)
        sums = jnp.dot(acts, part, preferred_element_type=F32)
        for s in range(low, high):
            p = s + 2 - frame
            for i, tap in enumerate(3 * q + k for q in taps for k in range(3)):
                rows = pl.ds((9 * p + tap) * chans, chans)
                block = sums[(s - low) * chans : (s - low + 1) * chans, i * chans : (i + 1) * chans]
                total[layer, rows, :] = block if s == 0 else total[layer, rows, :] + block

    half_at = lambda which: which * (share - half_rows)
    aligned = lambda value: pl.multiple_of(value, unit)
    settled = min(slots, -(-18 * chans // share))
    groups = [(low, high) for low, high in ((0, settled), (settled, slots)) if low < high]
    first_rows = -(-chunk // (2 * unit)) * unit
    parts = [(low, count) for low, count in ((0, first_rows), (first_rows, chunk - first_rows)) if count > 0]
    own_half = lambda slot: aligned(slot * share + half_at(core))

    def core_copy(layer, group):
        low, high = groups[group]
        range_ = pl.ds(low, high - low)
        return remote(
            core_out.at[layer, range_], core_in.at[layer, range_],
            core_send.at[layer, group], core_recv.at[layer, group], (t, 2 * lane + 1 - core),
        )

    def reduce_core(layer, group):
        for slot in range(*groups[group]):
            lines = pl.ds(aligned(slot * share + half_at(1 - core)), half_rows)
            core_out[layer, slot] = total[layer, lines, :].astype(wire)
        core_copy(layer, group).start()

    def cross_copy(layer, group, part, step):
        low, high = groups[group]
        line, count = parts[part]
        to = lax.rem(lane + step, lanes)
        return remote(
            cross_out.at[layer, pl.ds(low, high - low), pl.ds(aligned(to * chunk + line), count)],
            cross_in.at[layer, step - 1, pl.ds(low, high - low), pl.ds(line, count)],
            cross_send.at[layer, group, part, step - 1], cross_recv.at[layer, group, part, step - 1], (t, 2 * to + core),
        )

    def reduce_cross(layer, group):
        core_copy(layer, group).wait_recv()
        for slot in range(*groups[group]):
            cross_out[layer, slot] = (
                total[layer, pl.ds(own_half(slot), half_rows), :] + core_in[layer, slot].astype(F32)
            ).astype(wire)
        for part in range(len(parts)):
            for step in range(1, lanes):
                cross_copy(layer, group, part, step).start()

    def slot_copy(layer, part, step):
        to = lax.rem(t + step, slots)
        lines = pl.ds(*parts[part])
        return remote(
            slot_out.at[layer, to, lines], slot_in.at[layer, step - 1, lines],
            slot_send.at[layer, part, step - 1], slot_recv.at[layer, part, step - 1], (to, r),
        )

    def reduce_slots(layer, part):
        line, count = parts[part]
        for group in range(len(groups)):
            for step in range(1, lanes):
                cross_copy(layer, group, part, step).wait_recv()
        for slot in range(slots):
            mine = aligned(lane * chunk + line)
            value = total[layer, pl.ds(aligned(own_half(slot) + mine), count), :]
            value = value + core_in[layer, slot, pl.ds(mine, count), :].astype(F32)
            for step in range(1, lanes):
                value = value + cross_in[layer, step - 1, slot, pl.ds(line, count), :].astype(F32)
            slot_sum[layer, slot, pl.ds(line, count), :] = value
            slot_out[layer, slot, pl.ds(line, count), :] = value.astype(wire)
        for step in range(1, slots):
            slot_copy(layer, part, step).start()

    def band_copy(layer, part, step):
        to = lax.rem(r + step, bands)
        lines = pl.ds(*parts[part])
        return remote(
            band_in.at[layer, 0, lines], band_in.at[layer, step, lines],
            band_send.at[layer, part, step - 1], band_recv.at[layer, part, step - 1], (t, to),
        )

    def reduce_bands(layer, part):
        lines = pl.ds(*parts[part])
        for step in range(1, slots):
            slot_copy(layer, part, step).wait_recv()
        value = slot_sum[layer, t, lines, :]
        for step in range(1, slots):
            value = value + slot_in[layer, step - 1, lines, :].astype(F32)
        band_in[layer, 0, lines, :] = (value * factor).astype(wire)
        for step in range(1, bands):
            band_copy(layer, part, step).start()

    def finish(layer, target):
        for part in range(len(parts)):
            for step in range(1, bands):
                band_copy(layer, part, step).wait_recv()
        for band in range(bands):
            lines = pl.ds((band % 2) * (share - half_rows) + (band // 2) * chunk, chunk)
            target[lines, :] = band_in[layer, lax.rem(r - band + bands, bands)].astype(F32)

    def run(name, action, *args):
        with jax.named_scope(name):
            action(*args)

    chunks = height // step_rows
    late_frames = range(frames, frames + 2)

    zero = r // bands

    send_rows(1, up, 0, frames, 0)
    send_late(1, up)
    run("fill", fill_frames, 1, up, 0, frames)
    loads[1].wait()
    run("kernels", make_kernels, 1)
    loads[2].wait()
    run("active", make_active, 1)
    loads[3].wait()
    run("active", make_active, 0)
    loads[4].wait()
    run("kernels", make_kernels, 0)
    run("take_rows", take_rows, 1, up, 0, frames, 0)
    run("spread", spread, 1, 0, mid)
    send_rows(0, mid, 0, 2, 0)
    send_late(0, mid)
    run("fill", fill_frames, 0, mid, 0, 2)
    for frame in range(frames - 1):
        run("wsum", wsum, 1, frame)
    run("take_rows", take_rows, 0, mid, 0, 2, 0)
    for frame in range(2):
        run("wsum", wsum, 0, frame)
    run("fwd_late", forward_late, 1, up)
    run("wsum", wsum, 1, frames - 1)
    for frame in late_frames:
        run("wsum", wsum, 1, frame, (1,))
    run("edges", take_edges, 1)
    for pair in range(1, frames // 2):
        run("spread", spread, 1, pair, mid)
        send_rows(0, mid, 2 * pair, 2, pair)
    for frame in late_frames:
        run("wsum", wsum, 1, frame, (0, 2))
    for group in range(len(groups)):
        run("red_core", reduce_core, 1, group)
    run("fill", fill_frames, 0, mid, 2, frames)

    for frame in range(2, frames):
        run("wsum", wsum, 0, frame, (1,))
    for pair in range(1, frames // 2):
        run("take_rows", take_rows, 0, mid, 2 * pair, 2, pair)
    for group in range(len(groups)):
        run("red_cross", reduce_cross, 1, group)
    for frame in range(2, frames):
        run("wsum", wsum, 0, frame, (0, 2))
    if len(groups) > 1:
        run("red_core", reduce_core, 0, 1)
    run("fwd_late", forward_late, 0, mid)
    for frame in late_frames:
        run("wsum", wsum, 0, frame, (1,))
    if len(groups) > 1:
        run("red_cross", reduce_cross, 0, 1)
    run("spread", spread, 0, 0, out_ref, zero, zero + 1)
    run("edges", take_edges, 0)
    for frame in late_frames:
        run("wsum", wsum, 0, frame, (0, 2))
    run("red_core", reduce_core, 0, 0)
    for part in range(len(parts)):
        run("red_slots", reduce_slots, 1, part)
    run("spread", spread, 0, 0, out_ref, zero + 1, zero + chunks)
    run("red_cross", reduce_cross, 0, 0)
    for pair in range(1, frames // 2):
        run("spread", spread, 0, pair, out_ref)
    for part in range(len(parts)):
        run("red_slots", reduce_slots, 0, part)
    for part in range(len(parts)):
        run("red_bands", reduce_bands, 1, part)
    run("finish", finish, 1, grad_second_ref)
    for part in range(len(parts)):
        run("red_bands", reduce_bands, 0, part)
    run("finish", finish, 0, grad_first_ref)

    def sent(*copies):
        for copy in copies:
            copy.wait_send()

    when(has_above, lambda: sent(row_up(1, up, 0, frames, 0), *[row_up(0, mid, 2 * p, 2, p) for p in range(frames // 2)]))
    when(has_below, lambda: sent(row_down(1, up, 0, frames, 0), *[row_down(0, mid, 2 * p, 2, p) for p in range(frames // 2)]))
    when(has_prev, lambda: sent(*[late(1, up, f) for f in range(2)], *[late(0, mid, f) for f in range(2)]))
    for flag, copy in ((has_above, edge_up), (has_below, edge_down)):
        when(jnp.logical_and(has_later, flag), lambda copy=copy: sent(*[copy(layer, f) for layer in range(2) for f in range(2)]))
    for layer in range(2):
        for group in range(len(groups)):
            sent(core_copy(layer, group))
            sent(*[cross_copy(layer, group, part, step) for part in range(len(parts)) for step in range(1, lanes)])
        for part in range(len(parts)):
            sent(*[slot_copy(layer, part, step) for step in range(1, slots)])
            sent(*[band_copy(layer, part, step) for step in range(1, bands)])


def store_kernel(*refs):
    sources, targets, sems = refs[:3], refs[3:6], refs[6]
    copies = [pltpu.make_async_copy(src, dst, sems.at[i]) for i, (src, dst) in enumerate(zip(sources, targets))]
    for copy in copies:
        copy.start()
    for copy in copies:
        copy.wait()


def body(upstream, saved_first, saved_second, weight_first, weight_second):
    slots, bands = lax.axis_size("tm"), lax.axis_size("rows")
    frames, height, width, chans = upstream.shape
    depth = 27 * chans
    share, wire, unit, lanes, chunk, half_rows = plan(slots, bands, depth)
    factor = 1.0 / math.sqrt(frames * slots * height * bands * width)
    pairs = frames // 2
    vmem, dma = pltpu.VMEM, pltpu.SemaphoreType.DMA
    scratch = [
        vmem((frames, height, width, chans), BF16),
        vmem((2, frames, height, width, chans), BF16),
        vmem((2, depth, chans), BF16),
        vmem((frames, height, width, chans), BF16),
        vmem((2, frames + 2, (height + 2) * width, 3 * chans), BF16),
        vmem((2, frames, width, chans), BF16),
        vmem((2, frames, width, chans), BF16),
        vmem((2, 2, height, width, chans), BF16),
        vmem((2, 2, width, chans), BF16),
        vmem((2, 2, width, chans), BF16),
        vmem((2, 2 * chans, 36 * chans), BF16),
        vmem((2, frames * chans, height * width), BF16),
        vmem((2, depth, chans), F32),
        vmem((2, slots, half_rows, chans), wire),
        vmem((2, slots, half_rows, chans), wire),
        vmem((2, slots, half_rows, chans), wire),
        vmem((2, max(1, lanes - 1), slots, chunk, chans), wire),
        vmem((2, slots, chunk, chans), F32),
        vmem((2, slots, chunk, chans), wire),
        vmem((2, slots - 1, chunk, chans), wire),
        vmem((2, bands, chunk, chans), wire),
        dma((5,)),
        dma((2, pairs, 2)), dma((2, pairs, 2)),
        dma((2, 2)), dma((2, 2)),
        dma((2, 2, 2)), dma((2, 2, 2)),
        dma((2, 2)), dma((2, 2)),
        dma((2, 2, 2, max(1, lanes - 1))), dma((2, 2, 2, max(1, lanes - 1))),
        dma((2, 2, slots - 1)), dma((2, 2, slots - 1)),
        dma((2, 2, bands - 1)), dma((2, 2, bands - 1)),
    ]
    shapes = [(upstream.shape, BF16), ((share, chans), F32), ((share, chans), F32)]
    results = pl.pallas_call(
        functools.partial(whole_kernel, slots, bands, factor),
        out_shape=[pltpu.VMEM(shape, kind) for shape, kind in shapes],
        in_specs=[pl.BlockSpec(memory_space=pl.ANY)] * 5,
        out_specs=[pl.BlockSpec(memory_space=pltpu.VMEM)] * 3,
        scratch_shapes=scratch,
        compiler_params=pltpu.CompilerParams(vmem_limit_bytes=VMEM_LIMIT, collective_id=0, has_side_effects=True),
        name="whole",
    )(upstream, saved_first, saved_second, weight_first, weight_second)
    return pl.pallas_call(
        store_kernel,
        out_shape=[jax.ShapeDtypeStruct(shape, kind) for shape, kind in shapes],
        in_specs=[pl.BlockSpec(memory_space=pltpu.VMEM)] * 3,
        out_specs=[pl.BlockSpec(memory_space=pl.ANY)] * 3,
        scratch_shapes=[dma((3,))],
        compiler_params=pltpu.CompilerParams(vmem_limit_bytes=2 * 1024 * 1024),
        name="store",
    )(*results)


def solution(mesh):
    grid = P("tm", "rows", None, None)
    return jax.shard_map(
        body,
        mesh=mesh,
        in_specs=(grid, grid, grid, P(), P()),
        out_specs=(grid, P("tm", None), P("tm", None)),
        check_vma=False,
    )
```

```python
import functools
import math

import jax
import jax.numpy as jnp
from jax import lax
from jax.experimental import pallas as pl
from jax.experimental.pallas import tpu as pltpu
from jax.sharding import PartitionSpec as P

F32, BF16 = jnp.float32, jnp.bfloat16
VMEM_LIMIT = 52 * 1024 * 1024
MESH = pl.DeviceIdType.MESH


def plan(slots, bands, depth):
    share = depth // slots
    wire, unit = (BF16, 16) if share % 16 == 0 else (F32, 8)
    lanes = bands // 2
    chunk = -(-share // (bands * unit)) * unit
    return share, wire, unit, lanes, chunk, lanes * chunk


def whole_kernel(
    slots, bands, factor,
    up_hbm, first_hbm, second_hbm, weight_first_hbm, weight_second_hbm,
    out_ref, grad_first_ref, grad_second_ref,
    up, saved, weights, mid, wide, above, below, later, later_above, later_below, saved_above, saved_below, kernels, active, reach, total,
    core_out, core_in, cross_out, cross_in, slot_sum, slot_out, slot_in, band_in,
    load_sem, row_send, row_recv, late_send, late_recv, edge_send, edge_recv, seen_send, seen_recv,
    core_send, core_recv, cross_send, cross_recv, slot_send, slot_recv, band_send, band_recv,
):
    frames, height, width, chans = up.shape
    depth = 27 * chans
    share, wire, unit, lanes, chunk, half_rows = plan(slots, bands, depth)
    t, r = lax.axis_index("tm"), lax.axis_index("rows")
    core, lane = lax.rem(r, 2), r // 2
    has_above, has_below = r > 0, r < bands - 1
    has_prev, has_later = t > 0, t < slots - 1

    def remote(src, dst, send, recv, where):
        return pltpu.make_async_remote_copy(
            src_ref=src, dst_ref=dst, send_sem=send, recv_sem=recv, device_id=where, device_id_type=MESH
        )

    loads = [
        pltpu.make_async_copy(src, dst, load_sem.at[i])
        for i, (src, dst) in enumerate((
            (up_hbm, up), (weight_second_hbm, weights.at[1]), (second_hbm, saved.at[1]),
            (first_hbm, saved.at[0]), (weight_first_hbm, weights.at[0]),
        ))
    ]
    for load in loads:
        load.start()
    barrier = pltpu.get_barrier_semaphore()
    for step in range(1, bands):
        pl.semaphore_signal(barrier, inc=1, device_id=(t, lax.rem(r + step, bands)), device_id_type=MESH)
    for step in range(1, slots):
        pl.semaphore_signal(barrier, inc=1, device_id=(lax.rem(t + step, slots), r), device_id_type=MESH)
    loads[0].wait()
    pl.semaphore_wait(barrier, bands + slots - 2)

    def row_up(layer, grad, low, count, index):
        part = pl.ds(low, count)
        return remote(grad.at[part, 0], below.at[layer, part], row_send.at[layer, index, 0], row_recv.at[layer, index, 0], (t, r - 1))

    def row_down(layer, grad, low, count, index):
        part = pl.ds(low, count)
        return remote(grad.at[part, height - 1], above.at[layer, part], row_send.at[layer, index, 1], row_recv.at[layer, index, 1], (t, r + 1))

    def late(layer, grad, frame):
        return remote(grad.at[frame], later.at[layer, frame], late_send.at[layer, frame], late_recv.at[layer, frame], (t - 1, r))

    def edge_up(layer, frame):
        return remote(later.at[layer, frame, 0], later_below.at[layer, frame], edge_send.at[layer, frame, 0], edge_recv.at[layer, frame, 0], (t, r - 1))

    def edge_down(layer, frame):
        return remote(later.at[layer, frame, height - 1], later_above.at[layer, frame], edge_send.at[layer, frame, 1], edge_recv.at[layer, frame, 1], (t, r + 1))

    def seen_up():
        rows = saved.at[0, pl.ds(frames - 2, 2), 0]
        return remote(rows, saved_below, seen_send.at[0], seen_recv.at[0], (t, r - 1))

    def seen_down():
        rows = saved.at[0, pl.ds(frames - 2, 2), height - 1]
        return remote(rows, saved_above, seen_send.at[1], seen_recv.at[1], (t, r + 1))

    def when(flag, *actions):
        @pl.when(flag)
        def _():
            for action in actions:
                action()

    def send_rows(layer, grad, low, count, index):
        when(has_above, lambda: row_up(layer, grad, low, count, index).start())
        when(has_below, lambda: row_down(layer, grad, low, count, index).start())

    def send_late(layer, grad):
        when(has_prev, *[lambda f=f: late(layer, grad, f).start() for f in range(2)])

    place = lax.broadcasted_iota(jnp.int32, (width, chans), 0)

    def fill_row(layer, value, frame, row):
        spread = value.astype(F32)
        after = jnp.where(place == width - 1, 0.0, pltpu.roll(spread, width - 1, 0)).astype(BF16)
        before = jnp.where(place == 0, 0.0, pltpu.roll(spread, 1, 0)).astype(BF16)
        lines = pl.ds(row * width, width) if isinstance(row, int) else pl.ds(pl.multiple_of(row * width, width), width)
        wide[layer, frame, lines, pl.ds(0, chans)] = after
        wide[layer, frame, lines, pl.ds(chans, chans)] = value
        wide[layer, frame, lines, pl.ds(2 * chans, chans)] = before

    def zero_row(layer, frame, row):
        wide[layer, frame, pl.ds(row * width, width), :] = jnp.zeros((width, 3 * chans), BF16)

    def fill_frames(layer, grad, low, high, base=0):
        def one(row, carry):
            for frame in range(low, high):
                fill_row(layer, grad[frame - base, row], frame, row + 1)
            return carry

        lax.fori_loop(0, height, one, 0)

    def take_rows(layer, grad, low, count, index):
        def got_above():
            row_down(layer, grad, low, count, index).wait_recv()
            for frame in range(low, low + count):
                fill_row(layer, above[layer, frame], frame, 0)

        def got_below():
            row_up(layer, grad, low, count, index).wait_recv()
            for frame in range(low, low + count):
                fill_row(layer, below[layer, frame], frame, height + 1)

        when(has_above, got_above)
        when(has_below, got_below)
        when(jnp.logical_not(has_above), *[lambda f=f: zero_row(layer, f, 0) for f in range(low, low + count)])
        when(jnp.logical_not(has_below), *[lambda f=f: zero_row(layer, f, height + 1) for f in range(low, low + count)])

    def forward_late(layer, grad):
        def forward(frame):
            late(layer, grad, frame).wait_recv()
            when(has_above, lambda: edge_up(layer, frame).start())
            when(has_below, lambda: edge_down(layer, frame).start())
            fill_frames(layer, later.at[layer], frames + frame, frames + frame + 1, base=frames)

        when(has_later, *[lambda f=f: forward(f) for f in range(2)])

        @pl.when(jnp.logical_not(has_later))
        def _():
            for frame in range(2):
                wide[layer, frames + frame] = jnp.zeros(wide.shape[2:], BF16)

    def take_edges(layer):
        def edges(frame):
            def got_above():
                edge_down(layer, frame).wait_recv()
                fill_row(layer, later_above[layer, frame], frames + frame, 0)

            def got_below():
                edge_up(layer, frame).wait_recv()
                fill_row(layer, later_below[layer, frame], frames + frame, height + 1)

            when(has_above, got_above)
            when(has_below, got_below)
            when(jnp.logical_not(has_above), lambda: zero_row(layer, frames + frame, 0))
            when(jnp.logical_not(has_below), lambda: zero_row(layer, frames + frame, height + 1))

        when(has_later, *[lambda f=f: edges(f) for f in range(2)])

    def make_kernels(layer):
        span = 9 * chans
        for half in range(2):
            for j in range(4):
                p = 2 + half - j
                for tap in range(9):
                    block = (
                        weights[layer, pl.ds((9 * p + tap) * chans, chans), :]
                        if 0 <= p < 3
                        else jnp.zeros((chans, chans), BF16)
                    )
                    kernels[layer, pl.ds(half * chans, chans), pl.ds(j * span + tap * chans, chans)] = block

    def silu(value):
        value = value.astype(F32)
        return value * jax.nn.sigmoid(value)

    def make_active(layer):
        def one(frame, carry):
            for row in range(height):
                lines = pl.ds(pl.multiple_of(frame * chans, chans), chans)
                active[layer, lines, pl.ds(row * width, width)] = silu(saved[layer, frame, row]).T.astype(BF16)
            return carry

        lax.fori_loop(0, frames, one, 0)

    def send_seen():
        when(has_above, lambda: seen_up().start())
        when(has_below, lambda: seen_down().start())

    def make_reach():
        reach[:, pl.ds(width, height * width)] = active[0, pl.ds((frames - 2) * chans, 2 * chans), :]

        def take(copy, rows, base):
            copy().wait_recv()
            for frame in range(2):
                reach[pl.ds(frame * chans, chans), pl.ds(base, width)] = silu(rows[frame]).T.astype(BF16)

        def clear(base):
            reach[:, pl.ds(base, width)] = jnp.zeros((2 * chans, width), BF16)

        when(has_above, lambda: take(seen_down, saved_above, 0))
        when(has_below, lambda: take(seen_up, saved_below, (height + 1) * width))
        when(jnp.logical_not(has_above), lambda: clear(0))
        when(jnp.logical_not(has_below), lambda: clear((height + 1) * width))

    step_rows = math.gcd(4, height)
    lines = step_rows * width

    def spread(layer, pair, target, low=0, high=height // step_rows):
        def one(index, carry):
            pieces = [
                wide[layer, 2 * pair + j, pl.ds(pl.multiple_of(index * lines + (2 - q) * width, width), lines), :]
                for j in range(4)
                for q in range(3)
            ]
            sums = lax.dot_general(
                jnp.concatenate(pieces, axis=1), kernels[layer], (((1,), (1,)), ((), ())), preferred_element_type=F32
            )
            for half in range(2):
                rows = pl.ds(index * step_rows, step_rows)
                value = saved[layer, 2 * pair + half, rows].reshape(lines, chans).astype(F32)
                sigma = jax.nn.sigmoid(value)
                slope = sigma * (1.0 + value * (1.0 - sigma))
                result = sums[:, half * chans : (half + 1) * chans] * slope
                target[2 * pair + half, rows] = result.astype(BF16).reshape(step_rows, width, chans)
            return carry

        lax.fori_loop(low, high, one, 0)

    def wsum(layer, frame, taps=(0, 1, 2)):
        low, high = max(0, frame - 2), min(frames, frame + 1)
        acts = active[layer, pl.ds(low * chans, (high - low) * chans), :]
        part = jnp.concatenate([wide[layer, frame, pl.ds((2 - q) * width, height * width), :] for q in taps], axis=1)
        sums = jnp.dot(acts, part, preferred_element_type=F32)
        for s in range(low, high):
            p = s + 2 - frame
            for i, tap in enumerate(3 * q + k for q in taps for k in range(3)):
                rows = pl.ds((9 * p + tap) * chans, chans)
                block = sums[(s - low) * chans : (s - low + 1) * chans, i * chans : (i + 1) * chans]
                total[layer, rows, :] = block if s == 0 else total[layer, rows, :] + block

    def wsum_late(frame):
        count = frames + 2 - frame
        acts = pl.ds((2 - count) * chans, count * chans)
        lhs = jnp.concatenate([reach[acts, pl.ds(q * width, height * width)] for q in range(3)], axis=0)
        sums = jnp.dot(lhs, wide[0, frame, pl.ds(width, height * width), :], preferred_element_type=F32)
        for q in range(3):
            for i in range(count):
                p = frames - count + i + 2 - frame
                for k in range(3):
                    rows = pl.ds((9 * p + 3 * q + k) * chans, chans)
                    total[0, rows, :] += sums[(q * count + i) * chans : (q * count + i + 1) * chans, k * chans : (k + 1) * chans]

    half_at = lambda which: which * (share - half_rows)
    aligned = lambda value: pl.multiple_of(value, unit)
    settled = min(slots, -(-18 * chans // share))
    groups = [(low, high) for low, high in ((0, settled), (settled, slots)) if low < high]
    first_rows = -(-chunk // (2 * unit)) * unit
    parts = [(low, count) for low, count in ((0, first_rows), (first_rows, chunk - first_rows)) if count > 0]
    own_half = lambda slot: aligned(slot * share + half_at(core))

    def core_copy(layer, group):
        low, high = groups[group]
        range_ = pl.ds(low, high - low)
        return remote(
            core_out.at[layer, range_], core_in.at[layer, range_],
            core_send.at[layer, group], core_recv.at[layer, group], (t, 2 * lane + 1 - core),
        )

    def reduce_core(layer, group):
        for slot in range(*groups[group]):
            lines = pl.ds(aligned(slot * share + half_at(1 - core)), half_rows)
            core_out[layer, slot] = total[layer, lines, :].astype(wire)
        core_copy(layer, group).start()

    def cross_copy(layer, group, part, step):
        low, high = groups[group]
        line, count = parts[part]
        to = lax.rem(lane + step, lanes)
        return remote(
            cross_out.at[layer, pl.ds(low, high - low), pl.ds(aligned(to * chunk + line), count)],
            cross_in.at[layer, step - 1, pl.ds(low, high - low), pl.ds(line, count)],
            cross_send.at[layer, group, part, step - 1], cross_recv.at[layer, group, part, step - 1], (t, 2 * to + core),
        )

    def reduce_cross(layer, group, part):
        if part == 0:
            core_copy(layer, group).wait_recv()
        line, count = parts[part]
        for slot in range(*groups[group]):
            for to in range(lanes):
                lines = pl.ds(to * chunk + line, count)
                value = total[layer, pl.ds(aligned(own_half(slot) + to * chunk + line), count), :]
                cross_out[layer, slot, lines] = (value + core_in[layer, slot, lines].astype(F32)).astype(wire)
        for step in range(1, lanes):
            cross_copy(layer, group, part, step).start()

    def slot_copy(layer, part, step):
        to = lax.rem(t + step, slots)
        lines = pl.ds(*parts[part])
        return remote(
            slot_out.at[layer, to, lines], slot_in.at[layer, step - 1, lines],
            slot_send.at[layer, part, step - 1], slot_recv.at[layer, part, step - 1], (to, r),
        )

    def reduce_slots(layer, part):
        line, count = parts[part]
        for group in range(len(groups)):
            for step in range(1, lanes):
                cross_copy(layer, group, part, step).wait_recv()
        for slot in range(slots):
            mine = aligned(lane * chunk + line)
            value = total[layer, pl.ds(aligned(own_half(slot) + mine), count), :]
            value = value + core_in[layer, slot, pl.ds(mine, count), :].astype(F32)
            for step in range(1, lanes):
                value = value + cross_in[layer, step - 1, slot, pl.ds(line, count), :].astype(F32)
            slot_sum[layer, slot, pl.ds(line, count), :] = value
            slot_out[layer, slot, pl.ds(line, count), :] = value.astype(wire)
        for step in range(1, slots):
            slot_copy(layer, part, step).start()

    def band_copy(layer, part, step):
        to = lax.rem(r + step, bands)
        lines = pl.ds(*parts[part])
        return remote(
            band_in.at[layer, 0, lines], band_in.at[layer, step, lines],
            band_send.at[layer, part, step - 1], band_recv.at[layer, part, step - 1], (t, to),
        )

    def reduce_bands(layer, part):
        lines = pl.ds(*parts[part])
        for step in range(1, slots):
            slot_copy(layer, part, step).wait_recv()
        value = slot_sum[layer, t, lines, :]
        for step in range(1, slots):
            value = value + slot_in[layer, step - 1, lines, :].astype(F32)
        band_in[layer, 0, lines, :] = (value * factor).astype(wire)
        for step in range(1, bands):
            band_copy(layer, part, step).start()

    def finish(layer, target):
        for part in range(len(parts)):
            for step in range(1, bands):
                band_copy(layer, part, step).wait_recv()
        for band in range(bands):
            lines = pl.ds((band % 2) * (share - half_rows) + (band // 2) * chunk, chunk)
            target[lines, :] = band_in[layer, lax.rem(r - band + bands, bands)].astype(F32)

    def run(name, action, *args):
        with jax.named_scope(name):
            action(*args)

    chunks = height // step_rows
    late_frames = range(frames, frames + 2)

    zero = r // bands

    every_part = range(len(parts))
    late_group, settled_group = 0, (1 if len(groups) > 1 else None)

    def cross_all(layer, group):
        for part in every_part:
            reduce_cross(layer, group, part)

    send_rows(1, up, 0, frames, 0)
    send_late(1, up)
    run("fill", fill_frames, 1, up, 0, frames)
    loads[1].wait()
    run("kernels", make_kernels, 1)
    loads[2].wait()
    run("active", make_active, 1)
    loads[3].wait()
    send_seen()
    run("active", make_active, 0)
    loads[4].wait()
    run("kernels", make_kernels, 0)
    run("take_rows", take_rows, 1, up, 0, frames, 0)
    run("spread", spread, 1, 0, mid)
    send_rows(0, mid, 0, 2, 0)
    send_late(0, mid)
    run("fill", fill_frames, 0, mid, 0, 2)
    for frame in range(frames - 1):
        run("wsum", wsum, 1, frame)
    run("reach", make_reach)
    run("take_rows", take_rows, 0, mid, 0, 2, 0)
    for frame in range(2):
        run("wsum", wsum, 0, frame)
    run("fwd_late", forward_late, 1, up)
    run("wsum", wsum, 1, frames - 1)
    if settled_group:
        run("red_core", reduce_core, 1, settled_group)
    for frame in late_frames:
        run("wsum", wsum, 1, frame, (1,))
    run("edges", take_edges, 1)
    for pair in range(1, frames // 2):
        run("spread", spread, 1, pair, mid)
        send_rows(0, mid, 2 * pair, 2, pair)
    if settled_group:
        run("red_cross", cross_all, 1, settled_group)
    for frame in late_frames:
        run("wsum", wsum, 1, frame, (0, 2))
    run("red_core", reduce_core, 1, late_group)
    run("fill", fill_frames, 0, mid, 2, frames)

    for frame in range(2, frames):
        run("wsum", wsum, 0, frame, (1,))
    run("red_cross", cross_all, 1, late_group)
    for pair in range(1, frames // 2):
        run("take_rows", take_rows, 0, mid, 2 * pair, 2, pair)
    for frame in range(2, frames):
        run("wsum", wsum, 0, frame, (0, 2))
    if settled_group:
        run("red_core", reduce_core, 0, settled_group)
    run("fwd_late", forward_late, 0, mid)
    for frame in late_frames:
        run("wsum_late", wsum_late, frame)
    run("red_core", reduce_core, 0, late_group)
    if settled_group:
        run("red_cross", cross_all, 0, settled_group)
    for part in every_part:
        run("red_slots", reduce_slots, 1, part)
    run("spread", spread, 0, 0, out_ref, zero, zero + 1)
    run("red_cross", cross_all, 0, late_group)
    run("spread", spread, 0, 0, out_ref, zero + 1, zero + chunks)
    run("edges", take_edges, 0)
    for pair in range(1, frames // 2):
        run("spread", spread, 0, pair, out_ref, zero, zero + 1)
        run("red_slots", reduce_slots, 0, 0)
        run("spread", spread, 0, pair, out_ref, zero + 1, zero + chunks)
    for part in every_part[1:]:
        run("red_slots", reduce_slots, 0, part)
    for part in every_part:
        run("red_bands_b", reduce_bands, 1, part)
    for part in every_part:
        run("red_bands", reduce_bands, 0, part)
    run("finish_b", finish, 1, grad_second_ref)
    run("finish", finish, 0, grad_first_ref)

    def sent(*copies):
        for copy in copies:
            copy.wait_send()

    when(has_above, lambda: sent(row_up(1, up, 0, frames, 0), *[row_up(0, mid, 2 * p, 2, p) for p in range(frames // 2)]))
    when(has_below, lambda: sent(row_down(1, up, 0, frames, 0), *[row_down(0, mid, 2 * p, 2, p) for p in range(frames // 2)]))
    when(has_prev, lambda: sent(*[late(1, up, f) for f in range(2)], *[late(0, mid, f) for f in range(2)]))
    when(has_above, lambda: sent(seen_up()))
    when(has_below, lambda: sent(seen_down()))
    for flag, copy in ((has_above, edge_up), (has_below, edge_down)):
        when(jnp.logical_and(has_later, flag), lambda copy=copy: sent(*[copy(layer, f) for layer in range(2) for f in range(2)]))
    for layer in range(2):
        for group in range(len(groups)):
            sent(core_copy(layer, group))
            sent(*[cross_copy(layer, group, part, step) for part in range(len(parts)) for step in range(1, lanes)])
        for part in range(len(parts)):
            sent(*[slot_copy(layer, part, step) for step in range(1, slots)])
            sent(*[band_copy(layer, part, step) for step in range(1, bands)])


def store_kernel(*refs):
    sources, targets, sems = refs[:3], refs[3:6], refs[6]
    copies = [pltpu.make_async_copy(src, dst, sems.at[i]) for i, (src, dst) in enumerate(zip(sources, targets))]
    for copy in copies:
        copy.start()
    for copy in copies:
        copy.wait()


def body(upstream, saved_first, saved_second, weight_first, weight_second):
    slots, bands = lax.axis_size("tm"), lax.axis_size("rows")
    frames, height, width, chans = upstream.shape
    depth = 27 * chans
    share, wire, unit, lanes, chunk, half_rows = plan(slots, bands, depth)
    factor = 1.0 / math.sqrt(frames * slots * height * bands * width)
    pairs = frames // 2
    vmem, dma = pltpu.VMEM, pltpu.SemaphoreType.DMA
    scratch = [
        vmem((frames, height, width, chans), BF16),
        vmem((2, frames, height, width, chans), BF16),
        vmem((2, depth, chans), BF16),
        vmem((frames, height, width, chans), BF16),
        vmem((2, frames + 2, (height + 2) * width, 3 * chans), BF16),
        vmem((2, frames, width, chans), BF16),
        vmem((2, frames, width, chans), BF16),
        vmem((2, 2, height, width, chans), BF16),
        vmem((2, 2, width, chans), BF16),
        vmem((2, 2, width, chans), BF16),
        vmem((2, width, chans), BF16),
        vmem((2, width, chans), BF16),
        vmem((2, 2 * chans, 36 * chans), BF16),
        vmem((2, frames * chans, height * width), BF16),
        vmem((2 * chans, (height + 2) * width), BF16),
        vmem((2, depth, chans), F32),
        vmem((2, slots, half_rows, chans), wire),
        vmem((2, slots, half_rows, chans), wire),
        vmem((2, slots, half_rows, chans), wire),
        vmem((2, max(1, lanes - 1), slots, chunk, chans), wire),
        vmem((2, slots, chunk, chans), F32),
        vmem((2, slots, chunk, chans), wire),
        vmem((2, slots - 1, chunk, chans), wire),
        vmem((2, bands, chunk, chans), wire),
        dma((5,)),
        dma((2, pairs, 2)), dma((2, pairs, 2)),
        dma((2, 2)), dma((2, 2)),
        dma((2, 2, 2)), dma((2, 2, 2)),
        dma((2,)), dma((2,)),
        dma((2, 2)), dma((2, 2)),
        dma((2, 2, 2, max(1, lanes - 1))), dma((2, 2, 2, max(1, lanes - 1))),
        dma((2, 2, slots - 1)), dma((2, 2, slots - 1)),
        dma((2, 2, bands - 1)), dma((2, 2, bands - 1)),
    ]
    shapes = [(upstream.shape, BF16), ((share, chans), F32), ((share, chans), F32)]
    results = pl.pallas_call(
        functools.partial(whole_kernel, slots, bands, factor),
        out_shape=[pltpu.VMEM(shape, kind) for shape, kind in shapes],
        in_specs=[pl.BlockSpec(memory_space=pl.ANY)] * 5,
        out_specs=[pl.BlockSpec(memory_space=pltpu.VMEM)] * 3,
        scratch_shapes=scratch,
        compiler_params=pltpu.CompilerParams(vmem_limit_bytes=VMEM_LIMIT, collective_id=0, has_side_effects=True),
        name="whole",
    )(upstream, saved_first, saved_second, weight_first, weight_second)
    return pl.pallas_call(
        store_kernel,
        out_shape=[jax.ShapeDtypeStruct(shape, kind) for shape, kind in shapes],
        in_specs=[pl.BlockSpec(memory_space=pltpu.VMEM)] * 3,
        out_specs=[pl.BlockSpec(memory_space=pl.ANY)] * 3,
        scratch_shapes=[dma((3,))],
        compiler_params=pltpu.CompilerParams(vmem_limit_bytes=2 * 1024 * 1024),
        name="store",
    )(*results)


def solution(mesh):
    grid = P("tm", "rows", None, None)
    return jax.shard_map(
        body,
        mesh=mesh,
        in_specs=(grid, grid, grid, P(), P()),
        out_specs=(grid, P("tm", None), P("tm", None)),
        check_vma=False,
    )
```

```python
import functools
import math

import jax
import jax.numpy as jnp
from jax import lax
from jax.experimental import pallas as pl
from jax.experimental.pallas import tpu as pltpu
from jax.sharding import PartitionSpec as P

F32, BF16 = jnp.float32, jnp.bfloat16
VMEM_LIMIT = 52 * 1024 * 1024
PARTS = 2
MESH = pl.DeviceIdType.MESH


def plan(slots, bands, depth):
    share = depth // slots
    wire, unit = (BF16, 16) if share % 16 == 0 else (F32, 8)
    lanes = bands // 2
    chunk = -(-share // (bands * unit)) * unit
    return share, wire, unit, lanes, chunk, lanes * chunk


def whole_kernel(
    slots, bands, factor,
    up_hbm, first_hbm, second_hbm, weight_first_hbm, weight_second_hbm,
    out_ref, grad_first_ref, grad_second_ref,
    up, saved, weights, mid, wide, above, below, later, later_above, later_below, saved_above, saved_below, kernels, active, reach, total,
    core_out, core_in, cross_out, cross_in, slot_sum, slot_out, slot_in, band_in,
    load_sem, row_send, row_recv, late_send, late_recv, edge_send, edge_recv, seen_send, seen_recv,
    core_send, core_recv, cross_send, cross_recv, slot_send, slot_recv, band_send, band_recv,
):
    frames, height, width, chans = up.shape
    depth = 27 * chans
    share, wire, unit, lanes, chunk, half_rows = plan(slots, bands, depth)
    t, r = lax.axis_index("tm"), lax.axis_index("rows")
    core, lane = lax.rem(r, 2), r // 2
    has_above, has_below = r > 0, r < bands - 1
    has_prev, has_later = t > 0, t < slots - 1

    def remote(src, dst, send, recv, where):
        return pltpu.make_async_remote_copy(
            src_ref=src, dst_ref=dst, send_sem=send, recv_sem=recv, device_id=where, device_id_type=MESH
        )

    loads = [
        pltpu.make_async_copy(src, dst, load_sem.at[i])
        for i, (src, dst) in enumerate((
            (up_hbm, up), (weight_second_hbm, weights.at[1]), (second_hbm, saved.at[1]),
            (first_hbm, saved.at[0]), (weight_first_hbm, weights.at[0]),
        ))
    ]
    for load in loads:
        load.start()
    barrier = pltpu.get_barrier_semaphore()
    for step in range(1, bands):
        pl.semaphore_signal(barrier, inc=1, device_id=(t, lax.rem(r + step, bands)), device_id_type=MESH)
    for step in range(1, slots):
        pl.semaphore_signal(barrier, inc=1, device_id=(lax.rem(t + step, slots), r), device_id_type=MESH)
    loads[0].wait()
    pl.semaphore_wait(barrier, bands + slots - 2)

    def row_up(layer, grad, low, count, index):
        part = pl.ds(low, count)
        return remote(grad.at[part, 0], below.at[layer, part], row_send.at[layer, index, 0], row_recv.at[layer, index, 0], (t, r - 1))

    def row_down(layer, grad, low, count, index):
        part = pl.ds(low, count)
        return remote(grad.at[part, height - 1], above.at[layer, part], row_send.at[layer, index, 1], row_recv.at[layer, index, 1], (t, r + 1))

    def late(layer, grad, frame):
        return remote(grad.at[frame], later.at[layer, frame], late_send.at[layer, frame], late_recv.at[layer, frame], (t - 1, r))

    def edge_up(layer, frame):
        return remote(later.at[layer, frame, 0], later_below.at[layer, frame], edge_send.at[layer, frame, 0], edge_recv.at[layer, frame, 0], (t, r - 1))

    def edge_down(layer, frame):
        return remote(later.at[layer, frame, height - 1], later_above.at[layer, frame], edge_send.at[layer, frame, 1], edge_recv.at[layer, frame, 1], (t, r + 1))

    def seen_up(layer):
        rows = saved.at[layer, pl.ds(frames - 2, 2), 0]
        return remote(rows, saved_below.at[layer], seen_send.at[layer, 0], seen_recv.at[layer, 0], (t, r - 1))

    def seen_down(layer):
        rows = saved.at[layer, pl.ds(frames - 2, 2), height - 1]
        return remote(rows, saved_above.at[layer], seen_send.at[layer, 1], seen_recv.at[layer, 1], (t, r + 1))

    def when(flag, *actions):
        @pl.when(flag)
        def _():
            for action in actions:
                action()

    def send_rows(layer, grad, low, count, index):
        when(has_above, lambda: row_up(layer, grad, low, count, index).start())
        when(has_below, lambda: row_down(layer, grad, low, count, index).start())

    def send_late(layer, grad):
        when(has_prev, *[lambda f=f: late(layer, grad, f).start() for f in range(2)])

    place = lax.broadcasted_iota(jnp.int32, (width, chans), 0)

    def fill_row(layer, value, frame, row):
        spread = value.astype(F32)
        after = jnp.where(place == width - 1, 0.0, pltpu.roll(spread, width - 1, 0)).astype(BF16)
        before = jnp.where(place == 0, 0.0, pltpu.roll(spread, 1, 0)).astype(BF16)
        lines = pl.ds(row * width, width) if isinstance(row, int) else pl.ds(pl.multiple_of(row * width, width), width)
        wide[layer, frame, lines, pl.ds(0, chans)] = after
        wide[layer, frame, lines, pl.ds(chans, chans)] = value
        wide[layer, frame, lines, pl.ds(2 * chans, chans)] = before

    def zero_row(layer, frame, row):
        wide[layer, frame, pl.ds(row * width, width), :] = jnp.zeros((width, 3 * chans), BF16)

    def fill_frames(layer, grad, low, high, base=0):
        def one(row, carry):
            for frame in range(low, high):
                fill_row(layer, grad[frame - base, row], frame, row + 1)
            return carry

        lax.fori_loop(0, height, one, 0)

    def take_rows(layer, grad, low, count, index):
        def got_above():
            row_down(layer, grad, low, count, index).wait_recv()
            for frame in range(low, low + count):
                fill_row(layer, above[layer, frame], frame, 0)

        def got_below():
            row_up(layer, grad, low, count, index).wait_recv()
            for frame in range(low, low + count):
                fill_row(layer, below[layer, frame], frame, height + 1)

        when(has_above, got_above)
        when(has_below, got_below)
        when(jnp.logical_not(has_above), *[lambda f=f: zero_row(layer, f, 0) for f in range(low, low + count)])
        when(jnp.logical_not(has_below), *[lambda f=f: zero_row(layer, f, height + 1) for f in range(low, low + count)])

    def forward_late(layer, grad, frame):
        def forward():
            late(layer, grad, frame).wait_recv()
            when(has_above, lambda: edge_up(layer, frame).start())
            when(has_below, lambda: edge_down(layer, frame).start())
            fill_frames(layer, later.at[layer], frames + frame, frames + frame + 1, base=frames)

        def clear():
            wide[layer, frames + frame] = jnp.zeros(wide.shape[2:], BF16)

        when(has_later, forward)
        when(jnp.logical_not(has_later), clear)

    def take_edges(layer):
        def edges(frame):
            def got_above():
                edge_down(layer, frame).wait_recv()
                fill_row(layer, later_above[layer, frame], frames + frame, 0)

            def got_below():
                edge_up(layer, frame).wait_recv()
                fill_row(layer, later_below[layer, frame], frames + frame, height + 1)

            when(has_above, got_above)
            when(has_below, got_below)
            when(jnp.logical_not(has_above), lambda: zero_row(layer, frames + frame, 0))
            when(jnp.logical_not(has_below), lambda: zero_row(layer, frames + frame, height + 1))

        when(has_later, *[lambda f=f: edges(f) for f in range(2)])

    def make_kernels(layer):
        span = 9 * chans
        for half in range(2):
            for j in range(4):
                p = 2 + half - j
                for tap in range(9):
                    block = (
                        weights[layer, pl.ds((9 * p + tap) * chans, chans), :]
                        if 0 <= p < 3
                        else jnp.zeros((chans, chans), BF16)
                    )
                    kernels[layer, pl.ds(half * chans, chans), pl.ds(j * span + tap * chans, chans)] = block

    def silu(value):
        value = value.astype(F32)
        return value * jax.nn.sigmoid(value)

    def make_active(layer):
        def one(frame, carry):
            for row in range(height):
                lines = pl.ds(pl.multiple_of(frame * chans, chans), chans)
                active[layer, lines, pl.ds(row * width, width)] = silu(saved[layer, frame, row]).T.astype(BF16)
            return carry

        lax.fori_loop(0, frames, one, 0)

    def send_seen(layer):
        when(has_above, lambda: seen_up(layer).start())
        when(has_below, lambda: seen_down(layer).start())

    def make_reach(layer):
        reach[layer, :, pl.ds(width, height * width)] = active[layer, pl.ds((frames - 2) * chans, 2 * chans), :]

        def take(copy, rows, base):
            copy(layer).wait_recv()
            for frame in range(2):
                reach[layer, pl.ds(frame * chans, chans), pl.ds(base, width)] = silu(rows[layer, frame]).T.astype(BF16)

        def clear(base):
            reach[layer, :, pl.ds(base, width)] = jnp.zeros((2 * chans, width), BF16)

        when(has_above, lambda: take(seen_down, saved_above, 0))
        when(has_below, lambda: take(seen_up, saved_below, (height + 1) * width))
        when(jnp.logical_not(has_above), lambda: clear(0))
        when(jnp.logical_not(has_below), lambda: clear((height + 1) * width))

    step_rows = math.gcd(4, height)
    lines = step_rows * width

    def spread(layer, pair, target, low=0, high=height // step_rows):
        def one(index, carry):
            pieces = [
                wide[layer, 2 * pair + j, pl.ds(pl.multiple_of(index * lines + (2 - q) * width, width), lines), :]
                for j in range(4)
                for q in range(3)
            ]
            sums = lax.dot_general(
                jnp.concatenate(pieces, axis=1), kernels[layer], (((1,), (1,)), ((), ())), preferred_element_type=F32
            )
            for half in range(2):
                rows = pl.ds(index * step_rows, step_rows)
                value = saved[layer, 2 * pair + half, rows].reshape(lines, chans).astype(F32)
                sigma = jax.nn.sigmoid(value)
                slope = sigma * (1.0 + value * (1.0 - sigma))
                result = sums[:, half * chans : (half + 1) * chans] * slope
                target[2 * pair + half, rows] = result.astype(BF16).reshape(step_rows, width, chans)
            return carry

        lax.fori_loop(low, high, one, 0)

    def wsum(layer, frame, taps=(0, 1, 2)):
        low, high = max(0, frame - 2), min(frames, frame + 1)
        acts = active[layer, pl.ds(low * chans, (high - low) * chans), :]
        part = jnp.concatenate([wide[layer, frame, pl.ds((2 - q) * width, height * width), :] for q in taps], axis=1)
        sums = jnp.dot(acts, part, preferred_element_type=F32)
        for s in range(low, high):
            p = s + 2 - frame
            for i, tap in enumerate(3 * q + k for q in taps for k in range(3)):
                rows = pl.ds((9 * p + tap) * chans, chans)
                total[layer, rows, :] += sums[(s - low) * chans : (s - low + 1) * chans, i * chans : (i + 1) * chans]

    def wsum_late(layer, index):
        count = 2 - index
        acts = pl.ds(index * chans, count * chans)
        lhs = jnp.concatenate([reach[layer, acts, pl.ds(q * width, height * width)] for q in range(3)], axis=0)
        sums = jnp.dot(lhs, wide[layer, frames + index, pl.ds(width, height * width), :], preferred_element_type=F32)
        for q in range(3):
            for p in range(count):
                for k in range(3):
                    rows = pl.ds((9 * p + 3 * q + k) * chans, chans)
                    line = (q * count + p) * chans
                    total[layer, rows, :] += sums[line : line + chans, k * chans : (k + 1) * chans]

    half_at = lambda which: which * (share - half_rows)
    aligned = lambda value: pl.multiple_of(value, unit)
    settled = min(slots, -(-9 * chans // share))
    groups = [(low, high) for low, high in ((0, settled), (settled, slots)) if low < high]
    units = chunk // unit
    cuts = [units * i // PARTS * unit for i in range(PARTS + 1)]
    parts = [(low, high - low) for low, high in zip(cuts, cuts[1:]) if low < high]
    own_half = lambda slot: aligned(slot * share + half_at(core))

    def core_copy(layer, group):
        low, high = groups[group]
        range_ = pl.ds(low, high - low)
        return remote(
            core_out.at[layer, range_], core_in.at[layer, range_],
            core_send.at[layer, group], core_recv.at[layer, group], (t, 2 * lane + 1 - core),
        )

    def reduce_core(layer, group):
        for slot in range(*groups[group]):
            lines = pl.ds(aligned(slot * share + half_at(1 - core)), half_rows)
            core_out[layer, slot] = total[layer, lines, :].astype(wire)
        core_copy(layer, group).start()

    def cross_copy(layer, group, part, step):
        low, high = groups[group]
        line, count = parts[part]
        to = lax.rem(lane + step, lanes)
        return remote(
            cross_out.at[layer, pl.ds(low, high - low), pl.ds(aligned(to * chunk + line), count)],
            cross_in.at[layer, step - 1, pl.ds(low, high - low), pl.ds(line, count)],
            cross_send.at[layer, group, part, step - 1], cross_recv.at[layer, group, part, step - 1], (t, 2 * to + core),
        )

    def reduce_cross(layer, group, part):
        if part == 0:
            core_copy(layer, group).wait_recv()
        line, count = parts[part]
        for slot in range(*groups[group]):
            for to in range(lanes):
                lines = pl.ds(to * chunk + line, count)
                value = total[layer, pl.ds(aligned(own_half(slot) + to * chunk + line), count), :]
                cross_out[layer, slot, lines] = (value + core_in[layer, slot, lines].astype(F32)).astype(wire)
        for step in range(1, lanes):
            cross_copy(layer, group, part, step).start()

    def slot_copy(layer, part, step):
        to = lax.rem(t + step, slots)
        lines = pl.ds(*parts[part])
        return remote(
            slot_out.at[layer, to, lines], slot_in.at[layer, step - 1, lines],
            slot_send.at[layer, part, step - 1], slot_recv.at[layer, part, step - 1], (to, r),
        )

    def reduce_slots(layer, group, part):
        line, count = parts[part]
        low, high = groups[group]
        for step in range(1, lanes):
            cross_copy(layer, group, part, step).wait_recv()
        for slot in range(low, high):
            mine = aligned(lane * chunk + line)
            value = total[layer, pl.ds(aligned(own_half(slot) + mine), count), :]
            value = value + core_in[layer, slot, pl.ds(mine, count), :].astype(F32)
            for step in range(1, lanes):
                value = value + cross_in[layer, step - 1, slot, pl.ds(line, count), :].astype(F32)
            slot_sum[layer, slot, pl.ds(line, count), :] = value
            slot_out[layer, slot, pl.ds(line, count), :] = value.astype(wire)
        for step in range(1, slots):
            to = lax.rem(t + step, slots)
            when(jnp.logical_and(to >= low, to < high), lambda step=step: slot_copy(layer, part, step).start())

    def band_copy(layer, part, step):
        to = lax.rem(r + step, bands)
        lines = pl.ds(*parts[part])
        return remote(
            band_in.at[layer, 0, lines], band_in.at[layer, step, lines],
            band_send.at[layer, part, step - 1], band_recv.at[layer, part, step - 1], (t, to),
        )

    def reduce_bands(layer, part):
        lines = pl.ds(*parts[part])
        for step in range(1, slots):
            slot_copy(layer, part, step).wait_recv()
        value = slot_sum[layer, t, lines, :]
        for step in range(1, slots):
            value = value + slot_in[layer, step - 1, lines, :].astype(F32)
        band_in[layer, 0, lines, :] = (value * factor).astype(wire)
        for step in range(1, bands):
            band_copy(layer, part, step).start()

    def finish(layer, target):
        for part in range(len(parts)):
            for step in range(1, bands):
                band_copy(layer, part, step).wait_recv()
        for band in range(bands):
            lines = pl.ds((band % 2) * (share - half_rows) + (band // 2) * chunk, chunk)
            target[lines, :] = band_in[layer, lax.rem(r - band + bands, bands)].astype(F32)

    def run(name, action, *args):
        with jax.named_scope(name):
            action(*args)

    chunks = height // step_rows

    zero = r // bands

    every_part = range(len(parts))
    late_group, settled_group = 0, (1 if len(groups) > 1 else None)

    def cross_all(layer, group):
        for part in every_part:
            reduce_cross(layer, group, part)

    def clear_total():
        def one(index, carry):
            for layer in range(2):
                total[layer, pl.ds(pl.multiple_of(index * chans, chans), chans), :] = jnp.zeros((chans, chans), F32)
            return carry

        lax.fori_loop(0, 27, one, 0)

    send_rows(1, up, 0, frames, 0)
    send_late(1, up)
    run("fill", fill_frames, 1, up, 0, frames)
    loads[1].wait()
    run("kernels", make_kernels, 1)
    loads[2].wait()
    send_seen(1)
    run("active", make_active, 1)
    loads[3].wait()
    send_seen(0)
    run("active", make_active, 0)
    loads[4].wait()
    run("clear", clear_total)
    run("take_rows", take_rows, 1, up, 0, frames, 0)
    run("spread", spread, 1, 0, mid)
    send_rows(0, mid, 0, 2, 0)
    send_late(0, mid)
    run("fill", fill_frames, 0, mid, 0, 2)
    run("kernels", make_kernels, 0)
    for frame in range(frames):
        run("wsum", wsum, 1, frame)
    run("reach", make_reach, 1)
    run("reach", make_reach, 0)
    run("fwd_late", forward_late, 1, up, 0)
    run("wsum_late", wsum_late, 1, 0)
    if settled_group:
        run("red_core", reduce_core, 1, settled_group)
    run("fwd_late", forward_late, 1, up, 1)
    run("wsum_late", wsum_late, 1, 1)
    run("red_core", reduce_core, 1, late_group)
    run("take_rows", take_rows, 0, mid, 0, 2, 0)
    for frame in range(2):
        run("wsum", wsum, 0, frame)
    run("edges", take_edges, 1)
    if settled_group:
        run("red_cross", cross_all, 1, settled_group)
    for pair in range(1, frames // 2):
        run("spread", spread, 1, pair, mid)
        send_rows(0, mid, 2 * pair, 2, pair)
    run("red_cross", cross_all, 1, late_group)
    run("fill", fill_frames, 0, mid, 2, frames)

    for frame in range(2, frames):
        run("wsum", wsum, 0, frame, (1,))
    run("fwd_late", forward_late, 0, mid, 0)
    run("wsum_late", wsum_late, 0, 0)
    for pair in range(1, frames // 2):
        run("take_rows", take_rows, 0, mid, 2 * pair, 2, pair)
    for frame in range(2, frames):
        run("wsum", wsum, 0, frame, (0, 2))
    if settled_group:
        run("red_core", reduce_core, 0, settled_group)
    run("fwd_late", forward_late, 0, mid, 1)
    run("wsum_late", wsum_late, 0, 1)
    run("red_core", reduce_core, 0, late_group)
    if settled_group:
        run("red_cross_s", cross_all, 0, settled_group)
    for group in range(len(groups)):
        for part in every_part:
            run("red_slots_b", reduce_slots, 1, group, part)
    run("spread", spread, 0, 0, out_ref, zero, zero + 1)
    run("red_cross_l", cross_all, 0, late_group)
    run("spread", spread, 0, 0, out_ref, zero + 1, zero + chunks)
    run("edges", take_edges, 0)
    for pair in range(1, frames // 2):
        run("spread", spread, 0, pair, out_ref, zero, zero + 1)
    if settled_group:
        for part in every_part:
            run("red_slots_s", reduce_slots, 0, settled_group, part)
    for pair in range(1, frames // 2):
        run("spread", spread, 0, pair, out_ref, zero + 1, zero + chunks)
    for part in every_part:
        run("red_slots_l", reduce_slots, 0, late_group, part)
    for part in every_part:
        run("red_bands_b", reduce_bands, 1, part)
    for part in every_part:
        run("red_bands", reduce_bands, 0, part)
    run("finish_b", finish, 1, grad_second_ref)
    run("finish", finish, 0, grad_first_ref)

    def sent(*copies):
        for copy in copies:
            copy.wait_send()

    when(has_above, lambda: sent(row_up(1, up, 0, frames, 0), *[row_up(0, mid, 2 * p, 2, p) for p in range(frames // 2)]))
    when(has_below, lambda: sent(row_down(1, up, 0, frames, 0), *[row_down(0, mid, 2 * p, 2, p) for p in range(frames // 2)]))
    when(has_prev, lambda: sent(*[late(1, up, f) for f in range(2)], *[late(0, mid, f) for f in range(2)]))
    when(has_above, lambda: sent(seen_up(0), seen_up(1)))
    when(has_below, lambda: sent(seen_down(0), seen_down(1)))
    for flag, copy in ((has_above, edge_up), (has_below, edge_down)):
        when(jnp.logical_and(has_later, flag), lambda copy=copy: sent(*[copy(layer, f) for layer in range(2) for f in range(2)]))
    for layer in range(2):
        for group in range(len(groups)):
            sent(core_copy(layer, group))
            sent(*[cross_copy(layer, group, part, step) for part in range(len(parts)) for step in range(1, lanes)])
        for part in range(len(parts)):
            sent(*[slot_copy(layer, part, step) for step in range(1, slots)])
            sent(*[band_copy(layer, part, step) for step in range(1, bands)])


def store_kernel(*refs):
    sources, targets, sems = refs[:3], refs[3:6], refs[6]
    copies = [pltpu.make_async_copy(src, dst, sems.at[i]) for i, (src, dst) in enumerate(zip(sources, targets))]
    for copy in copies:
        copy.start()
    for copy in copies:
        copy.wait()


def body(upstream, saved_first, saved_second, weight_first, weight_second):
    slots, bands = lax.axis_size("tm"), lax.axis_size("rows")
    frames, height, width, chans = upstream.shape
    depth = 27 * chans
    share, wire, unit, lanes, chunk, half_rows = plan(slots, bands, depth)
    factor = 1.0 / math.sqrt(frames * slots * height * bands * width)
    pairs = frames // 2
    vmem, dma = pltpu.VMEM, pltpu.SemaphoreType.DMA
    scratch = [
        vmem((frames, height, width, chans), BF16),
        vmem((2, frames, height, width, chans), BF16),
        vmem((2, depth, chans), BF16),
        vmem((frames, height, width, chans), BF16),
        vmem((2, frames + 2, (height + 2) * width, 3 * chans), BF16),
        vmem((2, frames, width, chans), BF16),
        vmem((2, frames, width, chans), BF16),
        vmem((2, 2, height, width, chans), BF16),
        vmem((2, 2, width, chans), BF16),
        vmem((2, 2, width, chans), BF16),
        vmem((2, 2, width, chans), BF16),
        vmem((2, 2, width, chans), BF16),
        vmem((2, 2 * chans, 36 * chans), BF16),
        vmem((2, frames * chans, height * width), BF16),
        vmem((2, 2 * chans, (height + 2) * width), BF16),
        vmem((2, depth, chans), F32),
        vmem((2, slots, half_rows, chans), wire),
        vmem((2, slots, half_rows, chans), wire),
        vmem((2, slots, half_rows, chans), wire),
        vmem((2, max(1, lanes - 1), slots, chunk, chans), wire),
        vmem((2, slots, chunk, chans), F32),
        vmem((2, slots, chunk, chans), wire),
        vmem((2, slots - 1, chunk, chans), wire),
        vmem((2, bands, chunk, chans), wire),
        dma((5,)),
        dma((2, pairs, 2)), dma((2, pairs, 2)),
        dma((2, 2)), dma((2, 2)),
        dma((2, 2, 2)), dma((2, 2, 2)),
        dma((2, 2)), dma((2, 2)),
        dma((2, 2)), dma((2, 2)),
        dma((2, 2, PARTS, max(1, lanes - 1))), dma((2, 2, PARTS, max(1, lanes - 1))),
        dma((2, PARTS, slots - 1)), dma((2, PARTS, slots - 1)),
        dma((2, PARTS, bands - 1)), dma((2, PARTS, bands - 1)),
    ]
    shapes = [(upstream.shape, BF16), ((share, chans), F32), ((share, chans), F32)]
    results = pl.pallas_call(
        functools.partial(whole_kernel, slots, bands, factor),
        out_shape=[pltpu.VMEM(shape, kind) for shape, kind in shapes],
        in_specs=[pl.BlockSpec(memory_space=pl.ANY)] * 5,
        out_specs=[pl.BlockSpec(memory_space=pltpu.VMEM)] * 3,
        scratch_shapes=scratch,
        compiler_params=pltpu.CompilerParams(vmem_limit_bytes=VMEM_LIMIT, collective_id=0, has_side_effects=True),
        name="whole",
    )(upstream, saved_first, saved_second, weight_first, weight_second)
    return pl.pallas_call(
        store_kernel,
        out_shape=[jax.ShapeDtypeStruct(shape, kind) for shape, kind in shapes],
        in_specs=[pl.BlockSpec(memory_space=pltpu.VMEM)] * 3,
        out_specs=[pl.BlockSpec(memory_space=pl.ANY)] * 3,
        scratch_shapes=[dma((3,))],
        compiler_params=pltpu.CompilerParams(vmem_limit_bytes=2 * 1024 * 1024),
        name="store",
    )(*results)


def solution(mesh):
    grid = P("tm", "rows", None, None)
    return jax.shard_map(
        body,
        mesh=mesh,
        in_specs=(grid, grid, grid, P(), P()),
        out_specs=(grid, P("tm", None), P("tm", None)),
        check_vma=False,
    )
```

```python
import functools
import math

import jax
import jax.numpy as jnp
from jax import lax
from jax.experimental import pallas as pl
from jax.experimental.pallas import tpu as pltpu
from jax.sharding import PartitionSpec as P

F32, BF16 = jnp.float32, jnp.bfloat16
VMEM_LIMIT = 52 * 1024 * 1024
PARTS = 1
MESH = pl.DeviceIdType.MESH


def plan(slots, bands, depth):
    share = depth // slots
    wire, unit = (BF16, 16) if share % 16 == 0 else (F32, 8)
    lanes = bands // 2
    chunk = -(-share // (bands * unit)) * unit
    return share, wire, unit, lanes, chunk, lanes * chunk


def whole_kernel(
    slots, bands, factor,
    up_hbm, first_hbm, second_hbm, weight_first_hbm, weight_second_hbm,
    out_ref, grad_first_ref, grad_second_ref,
    up, saved, weights, mid, wide, above, below, later, later_above, later_below, saved_above, saved_below, kernels, active, reach, total,
    core_out, core_in, cross_out, cross_in, slot_sum, slot_out, slot_in, band_in,
    load_sem, row_send, row_recv, late_send, late_recv, edge_send, edge_recv, seen_send, seen_recv,
    core_send, core_recv, cross_send, cross_recv, slot_send, slot_recv, band_send, band_recv,
):
    frames, height, width, chans = up.shape
    depth = 27 * chans
    share, wire, unit, lanes, chunk, half_rows = plan(slots, bands, depth)
    t, r = lax.axis_index("tm"), lax.axis_index("rows")
    core, lane = lax.rem(r, 2), r // 2
    has_above, has_below = r > 0, r < bands - 1
    has_prev, has_later = t > 0, t < slots - 1

    def remote(src, dst, send, recv, where):
        return pltpu.make_async_remote_copy(
            src_ref=src, dst_ref=dst, send_sem=send, recv_sem=recv, device_id=where, device_id_type=MESH
        )

    loads = [
        pltpu.make_async_copy(src, dst, load_sem.at[i])
        for i, (src, dst) in enumerate((
            (up_hbm, up), (weight_second_hbm, weights.at[1]), (second_hbm, saved.at[1]),
            (first_hbm, saved.at[0]), (weight_first_hbm, weights.at[0]),
        ))
    ]
    for load in loads:
        load.start()
    barrier = pltpu.get_barrier_semaphore()
    for step in range(1, bands):
        pl.semaphore_signal(barrier, inc=1, device_id=(t, lax.rem(r + step, bands)), device_id_type=MESH)
    for step in range(1, slots):
        pl.semaphore_signal(barrier, inc=1, device_id=(lax.rem(t + step, slots), r), device_id_type=MESH)
    loads[0].wait()
    pl.semaphore_wait(barrier, bands + slots - 2)

    def row_up(layer, grad, low, count, index):
        part = pl.ds(low, count)
        return remote(grad.at[part, 0], below.at[layer, part], row_send.at[layer, index, 0], row_recv.at[layer, index, 0], (t, r - 1))

    def row_down(layer, grad, low, count, index):
        part = pl.ds(low, count)
        return remote(grad.at[part, height - 1], above.at[layer, part], row_send.at[layer, index, 1], row_recv.at[layer, index, 1], (t, r + 1))

    def late(layer, grad, frame):
        return remote(grad.at[frame], later.at[layer, frame], late_send.at[layer, frame], late_recv.at[layer, frame], (t - 1, r))

    def edge_up(layer, frame):
        return remote(later.at[layer, frame, 0], later_below.at[layer, frame], edge_send.at[layer, frame, 0], edge_recv.at[layer, frame, 0], (t, r - 1))

    def edge_down(layer, frame):
        return remote(later.at[layer, frame, height - 1], later_above.at[layer, frame], edge_send.at[layer, frame, 1], edge_recv.at[layer, frame, 1], (t, r + 1))

    def seen_up(layer):
        rows = saved.at[layer, :, 0]
        return remote(rows, saved_below.at[layer], seen_send.at[layer, 0], seen_recv.at[layer, 0], (t, r - 1))

    def seen_down(layer):
        rows = saved.at[layer, :, height - 1]
        return remote(rows, saved_above.at[layer], seen_send.at[layer, 1], seen_recv.at[layer, 1], (t, r + 1))

    def when(flag, *actions):
        @pl.when(flag)
        def _():
            for action in actions:
                action()

    def send_rows(layer, grad, low, count, index):
        when(has_above, lambda: row_up(layer, grad, low, count, index).start())
        when(has_below, lambda: row_down(layer, grad, low, count, index).start())

    def send_late(layer, grad):
        when(has_prev, *[lambda f=f: late(layer, grad, f).start() for f in range(2)])

    place = lax.broadcasted_iota(jnp.int32, (width, chans), 0)

    def fill_row(layer, value, frame, row):
        spread = value.astype(F32)
        after = jnp.where(place == width - 1, 0.0, pltpu.roll(spread, width - 1, 0)).astype(BF16)
        before = jnp.where(place == 0, 0.0, pltpu.roll(spread, 1, 0)).astype(BF16)
        lines = pl.ds(row * width, width) if isinstance(row, int) else pl.ds(pl.multiple_of(row * width, width), width)
        wide[layer, frame, lines, pl.ds(0, chans)] = after
        wide[layer, frame, lines, pl.ds(chans, chans)] = value
        wide[layer, frame, lines, pl.ds(2 * chans, chans)] = before

    def zero_row(layer, frame, row):
        wide[layer, frame, pl.ds(row * width, width), :] = jnp.zeros((width, 3 * chans), BF16)

    def fill_frames(layer, grad, low, high, base=0):
        def one(row, carry):
            for frame in range(low, high):
                fill_row(layer, grad[frame - base, row], frame, row + 1)
            return carry

        lax.fori_loop(0, height, one, 0)

    def take_rows(layer, grad, low, count, index):
        def got_above():
            row_down(layer, grad, low, count, index).wait_recv()
            for frame in range(low, low + count):
                fill_row(layer, above[layer, frame], frame, 0)

        def got_below():
            row_up(layer, grad, low, count, index).wait_recv()
            for frame in range(low, low + count):
                fill_row(layer, below[layer, frame], frame, height + 1)

        when(has_above, got_above)
        when(has_below, got_below)
        when(jnp.logical_not(has_above), *[lambda f=f: zero_row(layer, f, 0) for f in range(low, low + count)])
        when(jnp.logical_not(has_below), *[lambda f=f: zero_row(layer, f, height + 1) for f in range(low, low + count)])

    def forward_late(layer, grad, frame):
        def forward():
            late(layer, grad, frame).wait_recv()
            when(has_above, lambda: edge_up(layer, frame).start())
            when(has_below, lambda: edge_down(layer, frame).start())
            fill_frames(layer, later.at[layer], frames + frame, frames + frame + 1, base=frames)

        def clear():
            wide[layer, frames + frame] = jnp.zeros(wide.shape[2:], BF16)

        when(has_later, forward)
        when(jnp.logical_not(has_later), clear)

    def take_edges(layer):
        def edges(frame):
            def got_above():
                edge_down(layer, frame).wait_recv()
                fill_row(layer, later_above[layer, frame], frames + frame, 0)

            def got_below():
                edge_up(layer, frame).wait_recv()
                fill_row(layer, later_below[layer, frame], frames + frame, height + 1)

            when(has_above, got_above)
            when(has_below, got_below)
            when(jnp.logical_not(has_above), lambda: zero_row(layer, frames + frame, 0))
            when(jnp.logical_not(has_below), lambda: zero_row(layer, frames + frame, height + 1))

        when(has_later, *[lambda f=f: edges(f) for f in range(2)])

    def make_kernels(layer):
        span = 9 * chans
        for half in range(2):
            for j in range(4):
                p = 2 + half - j
                for tap in range(9):
                    block = (
                        weights[layer, pl.ds((9 * p + tap) * chans, chans), :]
                        if 0 <= p < 3
                        else jnp.zeros((chans, chans), BF16)
                    )
                    kernels[layer, pl.ds(half * chans, chans), pl.ds(j * span + tap * chans, chans)] = block

    def silu(value):
        value = value.astype(F32)
        return value * jax.nn.sigmoid(value)

    def make_active(layer):
        def one(frame, carry):
            for row in range(height):
                lines = pl.ds(pl.multiple_of(frame * chans, chans), chans)
                active[layer, lines, pl.ds(row * width, width)] = silu(saved[layer, frame, row]).T.astype(BF16)
            return carry

        lax.fori_loop(0, frames, one, 0)

    def send_seen(layer):
        when(has_above, lambda: seen_up(layer).start())
        when(has_below, lambda: seen_down(layer).start())

    def make_reach(layer):
        reach[layer, :, pl.ds(width, height * width)] = active[layer]

        def take(copy, rows, base):
            copy(layer).wait_recv()
            for frame in range(frames):
                reach[layer, pl.ds(frame * chans, chans), pl.ds(base, width)] = silu(rows[layer, frame]).T.astype(BF16)

        def clear(base):
            reach[layer, :, pl.ds(base, width)] = jnp.zeros((frames * chans, width), BF16)

        when(has_above, lambda: take(seen_down, saved_above, 0))
        when(has_below, lambda: take(seen_up, saved_below, (height + 1) * width))
        when(jnp.logical_not(has_above), lambda: clear(0))
        when(jnp.logical_not(has_below), lambda: clear((height + 1) * width))

    step_rows = math.gcd(4, height)
    lines = step_rows * width

    def spread(layer, pair, target, low=0, high=height // step_rows):
        def one(index, carry):
            pieces = [
                wide[layer, 2 * pair + j, pl.ds(pl.multiple_of(index * lines + (2 - q) * width, width), lines), :]
                for j in range(4)
                for q in range(3)
            ]
            sums = lax.dot_general(
                jnp.concatenate(pieces, axis=1), kernels[layer], (((1,), (1,)), ((), ())), preferred_element_type=F32
            )
            for half in range(2):
                rows = pl.ds(index * step_rows, step_rows)
                value = saved[layer, 2 * pair + half, rows].reshape(lines, chans).astype(F32)
                sigma = jax.nn.sigmoid(value)
                slope = sigma * (1.0 + value * (1.0 - sigma))
                result = sums[:, half * chans : (half + 1) * chans] * slope
                target[2 * pair + half, rows] = result.astype(BF16).reshape(step_rows, width, chans)
            return carry

        lax.fori_loop(low, high, one, 0)

    def wsum(layer, frame, taps=(0, 1, 2)):
        low, high = max(0, frame - 2), min(frames, frame + 1)
        acts = active[layer, pl.ds(low * chans, (high - low) * chans), :]
        part = jnp.concatenate([wide[layer, frame, pl.ds((2 - q) * width, height * width), :] for q in taps], axis=1)
        sums = jnp.dot(acts, part, preferred_element_type=F32)
        for s in range(low, high):
            p = s + 2 - frame
            for i, tap in enumerate(3 * q + k for q in taps for k in range(3)):
                rows = pl.ds((9 * p + tap) * chans, chans)
                total[layer, rows, :] += sums[(s - low) * chans : (s - low + 1) * chans, i * chans : (i + 1) * chans]

    def wsum_own(layer, frame):
        low, high = max(0, frame - 2), min(frames, frame + 1)
        count = high - low
        acts = pl.ds(low * chans, count * chans)
        lhs = jnp.concatenate([reach[layer, acts, pl.ds(q * width, height * width)] for q in range(3)], axis=0)
        sums = jnp.dot(lhs, wide[layer, frame, pl.ds(width, height * width), :], preferred_element_type=F32)
        for q in range(3):
            for i in range(count):
                p = low + i + 2 - frame
                for k in range(3):
                    rows = pl.ds((9 * p + 3 * q + k) * chans, chans)
                    line = (q * count + i) * chans
                    total[layer, rows, :] += sums[line : line + chans, k * chans : (k + 1) * chans]

    half_at = lambda which: which * (share - half_rows)
    aligned = lambda value: pl.multiple_of(value, unit)
    settled = min(slots, -(-9 * chans // share))
    groups = [(low, high) for low, high in ((0, settled), (settled, slots)) if low < high]
    units = chunk // unit
    cuts = [units * i // PARTS * unit for i in range(PARTS + 1)]
    parts = [(low, high - low) for low, high in zip(cuts, cuts[1:]) if low < high]
    own_half = lambda slot: aligned(slot * share + half_at(core))

    def core_copy(layer, group):
        low, high = groups[group]
        range_ = pl.ds(low, high - low)
        return remote(
            core_out.at[layer, range_], core_in.at[layer, range_],
            core_send.at[layer, group], core_recv.at[layer, group], (t, 2 * lane + 1 - core),
        )

    def reduce_core(layer, group):
        for slot in range(*groups[group]):
            lines = pl.ds(aligned(slot * share + half_at(1 - core)), half_rows)
            core_out[layer, slot] = total[layer, lines, :].astype(wire)
        core_copy(layer, group).start()

    def cross_copy(layer, group, part, step):
        low, high = groups[group]
        line, count = parts[part]
        to = lax.rem(lane + step, lanes)
        return remote(
            cross_out.at[layer, pl.ds(low, high - low), pl.ds(aligned(to * chunk + line), count)],
            cross_in.at[layer, step - 1, pl.ds(low, high - low), pl.ds(line, count)],
            cross_send.at[layer, group, part, step - 1], cross_recv.at[layer, group, part, step - 1], (t, 2 * to + core),
        )

    def reduce_cross(layer, group, part):
        if part == 0:
            core_copy(layer, group).wait_recv()
        line, count = parts[part]
        for slot in range(*groups[group]):
            for to in range(lanes):
                lines = pl.ds(to * chunk + line, count)
                value = total[layer, pl.ds(aligned(own_half(slot) + to * chunk + line), count), :]
                cross_out[layer, slot, lines] = (value + core_in[layer, slot, lines].astype(F32)).astype(wire)
        for step in range(1, lanes):
            cross_copy(layer, group, part, step).start()

    def slot_copy(layer, part, step):
        to = lax.rem(t + step, slots)
        lines = pl.ds(*parts[part])
        return remote(
            slot_out.at[layer, to, lines], slot_in.at[layer, step - 1, lines],
            slot_send.at[layer, part, step - 1], slot_recv.at[layer, part, step - 1], (to, r),
        )

    def reduce_slots(layer, group, part):
        line, count = parts[part]
        low, high = groups[group]
        for step in range(1, lanes):
            cross_copy(layer, group, part, step).wait_recv()
        for slot in range(low, high):
            mine = aligned(lane * chunk + line)
            value = total[layer, pl.ds(aligned(own_half(slot) + mine), count), :]
            value = value + core_in[layer, slot, pl.ds(mine, count), :].astype(F32)
            for step in range(1, lanes):
                value = value + cross_in[layer, step - 1, slot, pl.ds(line, count), :].astype(F32)
            slot_sum[layer, slot, pl.ds(line, count), :] = value
            slot_out[layer, slot, pl.ds(line, count), :] = value.astype(wire)
        for step in range(1, slots):
            to = lax.rem(t + step, slots)
            when(jnp.logical_and(to >= low, to < high), lambda step=step: slot_copy(layer, part, step).start())

    def band_copy(layer, part, step):
        to = lax.rem(r + step, bands)
        lines = pl.ds(*parts[part])
        return remote(
            band_in.at[layer, 0, lines], band_in.at[layer, step, lines],
            band_send.at[layer, part, step - 1], band_recv.at[layer, part, step - 1], (t, to),
        )

    def reduce_bands(layer, part):
        lines = pl.ds(*parts[part])
        for step in range(1, slots):
            slot_copy(layer, part, step).wait_recv()
        value = slot_sum[layer, t, lines, :]
        for step in range(1, slots):
            value = value + slot_in[layer, step - 1, lines, :].astype(F32)
        band_in[layer, 0, lines, :] = (value * factor).astype(wire)
        for step in range(1, bands):
            band_copy(layer, part, step).start()

    def finish(layer, target):
        for part in range(len(parts)):
            for step in range(1, bands):
                band_copy(layer, part, step).wait_recv()
        for band in range(bands):
            lines = pl.ds((band % 2) * (share - half_rows) + (band // 2) * chunk, chunk)
            target[lines, :] = band_in[layer, lax.rem(r - band + bands, bands)].astype(F32)

    def run(name, action, *args):
        with jax.named_scope(name):
            action(*args)

    chunks = height // step_rows

    zero = r // bands

    every_part = range(len(parts))
    late_group, settled_group = 0, (1 if len(groups) > 1 else None)

    def cross_all(layer, group):
        for part in every_part:
            reduce_cross(layer, group, part)

    def clear_total():
        def one(index, carry):
            for layer in range(2):
                total[layer, pl.ds(pl.multiple_of(index * chans, chans), chans), :] = jnp.zeros((chans, chans), F32)
            return carry

        lax.fori_loop(0, 27, one, 0)

    send_rows(1, up, 0, frames, 0)
    send_late(1, up)
    run("fill", fill_frames, 1, up, 0, frames)
    loads[1].wait()
    run("kernels", make_kernels, 1)
    loads[2].wait()
    send_seen(1)
    run("active", make_active, 1)
    loads[3].wait()
    send_seen(0)
    run("active", make_active, 0)
    loads[4].wait()
    run("clear", clear_total)
    run("take_rows", take_rows, 1, up, 0, frames, 0)
    run("spread", spread, 1, 0, mid)
    send_rows(0, mid, 0, 2, 0)
    send_late(0, mid)
    run("fill", fill_frames, 0, mid, 0, 2)
    run("kernels", make_kernels, 0)
    for frame in range(frames):
        run("wsum", wsum, 1, frame)
    run("reach", make_reach, 1)
    run("reach", make_reach, 0)
    run("fwd_late", forward_late, 1, up, 0)
    run("wsum_late", wsum_own, 1, frames + 0)
    if settled_group:
        run("red_core", reduce_core, 1, settled_group)
    run("fwd_late", forward_late, 1, up, 1)
    run("wsum_late", wsum_own, 1, frames + 1)
    run("red_core", reduce_core, 1, late_group)
    run("take_rows", take_rows, 0, mid, 0, 2, 0)
    for frame in range(2):
        run("wsum", wsum, 0, frame)
    run("edges", take_edges, 1)
    if settled_group:
        run("red_cross", cross_all, 1, settled_group)
    for pair in range(1, frames // 2):
        run("spread", spread, 1, pair, mid)
        send_rows(0, mid, 2 * pair, 2, pair)
    run("red_cross", cross_all, 1, late_group)
    run("fill", fill_frames, 0, mid, 2, frames)

    for frame in range(2, frames):
        run("wsum_own", wsum_own, 0, frame)
    run("fwd_late", forward_late, 0, mid, 0)
    run("wsum_late", wsum_own, 0, frames + 0)
    if settled_group:
        run("red_core", reduce_core, 0, settled_group)
    run("fwd_late", forward_late, 0, mid, 1)
    run("wsum_late", wsum_own, 0, frames + 1)
    run("red_core", reduce_core, 0, late_group)
    if settled_group:
        run("red_cross_s", cross_all, 0, settled_group)
    for group in range(len(groups)):
        for part in every_part:
            run("red_slots_b", reduce_slots, 1, group, part)
    for pair in range(1, frames // 2):
        run("take_rows", take_rows, 0, mid, 2 * pair, 2, pair)
    run("spread", spread, 0, 0, out_ref, zero, zero + 1)
    run("red_cross_l", cross_all, 0, late_group)
    run("spread", spread, 0, 0, out_ref, zero + 1, zero + chunks)
    run("edges", take_edges, 0)
    for pair in range(1, frames // 2):
        run("spread", spread, 0, pair, out_ref, zero, zero + 1)
    if settled_group:
        for part in every_part:
            run("red_slots_s", reduce_slots, 0, settled_group, part)
    for pair in range(1, frames // 2):
        run("spread", spread, 0, pair, out_ref, zero + 1, zero + chunks)
    for part in every_part:
        run("red_slots_l", reduce_slots, 0, late_group, part)
    for part in every_part:
        run("red_bands_b", reduce_bands, 1, part)
    for part in every_part:
        run("red_bands", reduce_bands, 0, part)
    run("finish_b", finish, 1, grad_second_ref)
    run("finish", finish, 0, grad_first_ref)

    def sent(*copies):
        for copy in copies:
            copy.wait_send()

    when(has_above, lambda: sent(row_up(1, up, 0, frames, 0), *[row_up(0, mid, 2 * p, 2, p) for p in range(frames // 2)]))
    when(has_below, lambda: sent(row_down(1, up, 0, frames, 0), *[row_down(0, mid, 2 * p, 2, p) for p in range(frames // 2)]))
    when(has_prev, lambda: sent(*[late(1, up, f) for f in range(2)], *[late(0, mid, f) for f in range(2)]))
    when(has_above, lambda: sent(seen_up(0), seen_up(1)))
    when(has_below, lambda: sent(seen_down(0), seen_down(1)))
    for flag, copy in ((has_above, edge_up), (has_below, edge_down)):
        when(jnp.logical_and(has_later, flag), lambda copy=copy: sent(*[copy(layer, f) for layer in range(2) for f in range(2)]))
    for layer in range(2):
        for group in range(len(groups)):
            sent(core_copy(layer, group))
            sent(*[cross_copy(layer, group, part, step) for part in range(len(parts)) for step in range(1, lanes)])
        for part in range(len(parts)):
            sent(*[slot_copy(layer, part, step) for step in range(1, slots)])
            sent(*[band_copy(layer, part, step) for step in range(1, bands)])


def store_kernel(*refs):
    sources, targets, sems = refs[:3], refs[3:6], refs[6]
    copies = [pltpu.make_async_copy(src, dst, sems.at[i]) for i, (src, dst) in enumerate(zip(sources, targets))]
    for copy in copies:
        copy.start()
    for copy in copies:
        copy.wait()


def body(upstream, saved_first, saved_second, weight_first, weight_second):
    slots, bands = lax.axis_size("tm"), lax.axis_size("rows")
    frames, height, width, chans = upstream.shape
    depth = 27 * chans
    share, wire, unit, lanes, chunk, half_rows = plan(slots, bands, depth)
    factor = 1.0 / math.sqrt(frames * slots * height * bands * width)
    pairs = frames // 2
    vmem, dma = pltpu.VMEM, pltpu.SemaphoreType.DMA
    scratch = [
        vmem((frames, height, width, chans), BF16),
        vmem((2, frames, height, width, chans), BF16),
        vmem((2, depth, chans), BF16),
        vmem((frames, height, width, chans), BF16),
        vmem((2, frames + 2, (height + 2) * width, 3 * chans), BF16),
        vmem((2, frames, width, chans), BF16),
        vmem((2, frames, width, chans), BF16),
        vmem((2, 2, height, width, chans), BF16),
        vmem((2, 2, width, chans), BF16),
        vmem((2, 2, width, chans), BF16),
        vmem((2, frames, width, chans), BF16),
        vmem((2, frames, width, chans), BF16),
        vmem((2, 2 * chans, 36 * chans), BF16),
        vmem((2, frames * chans, height * width), BF16),
        vmem((2, frames * chans, (height + 2) * width), BF16),
        vmem((2, depth, chans), F32),
        vmem((2, slots, half_rows, chans), wire),
        vmem((2, slots, half_rows, chans), wire),
        vmem((2, slots, half_rows, chans), wire),
        vmem((2, max(1, lanes - 1), slots, chunk, chans), wire),
        vmem((2, slots, chunk, chans), F32),
        vmem((2, slots, chunk, chans), wire),
        vmem((2, slots - 1, chunk, chans), wire),
        vmem((2, bands, chunk, chans), wire),
        dma((5,)),
        dma((2, pairs, 2)), dma((2, pairs, 2)),
        dma((2, 2)), dma((2, 2)),
        dma((2, 2, 2)), dma((2, 2, 2)),
        dma((2, 2)), dma((2, 2)),
        dma((2, 2)), dma((2, 2)),
        dma((2, 2, PARTS, max(1, lanes - 1))), dma((2, 2, PARTS, max(1, lanes - 1))),
        dma((2, PARTS, slots - 1)), dma((2, PARTS, slots - 1)),
        dma((2, PARTS, bands - 1)), dma((2, PARTS, bands - 1)),
    ]
    shapes = [(upstream.shape, BF16), ((share, chans), F32), ((share, chans), F32)]
    results = pl.pallas_call(
        functools.partial(whole_kernel, slots, bands, factor),
        out_shape=[pltpu.VMEM(shape, kind) for shape, kind in shapes],
        in_specs=[pl.BlockSpec(memory_space=pl.ANY)] * 5,
        out_specs=[pl.BlockSpec(memory_space=pltpu.VMEM)] * 3,
        scratch_shapes=scratch,
        compiler_params=pltpu.CompilerParams(vmem_limit_bytes=VMEM_LIMIT, collective_id=0, has_side_effects=True),
        name="whole",
    )(upstream, saved_first, saved_second, weight_first, weight_second)
    return pl.pallas_call(
        store_kernel,
        out_shape=[jax.ShapeDtypeStruct(shape, kind) for shape, kind in shapes],
        in_specs=[pl.BlockSpec(memory_space=pltpu.VMEM)] * 3,
        out_specs=[pl.BlockSpec(memory_space=pl.ANY)] * 3,
        scratch_shapes=[dma((3,))],
        compiler_params=pltpu.CompilerParams(vmem_limit_bytes=2 * 1024 * 1024),
        name="store",
    )(*results)


def solution(mesh):
    grid = P("tm", "rows", None, None)
    return jax.shard_map(
        body,
        mesh=mesh,
        in_specs=(grid, grid, grid, P(), P()),
        out_specs=(grid, P("tm", None), P("tm", None)),
        check_vma=False,
    )
```
